128 devices in a mesh: batch: 1, ysp: 64 (over z, y, x), xsp: 2 (over core).
Axes of the slice: x: 4, y: 4, z: 4, core: 2. Of those that a mesh axis runs over, the one named last changes fastest.
Arguments:
- volume: bfloat16 [64, 64, 2048, 32], P('batch', 'xsp', 'ysp')
- filter_taps: float32 [3, 3, 21], replicated
- mix_weights: bfloat16 [3, 64, 64], replicated
- mix_bias: float32 [3, 64], replicated
Outputs:
- output: bfloat16 [64, 64, 2048, 32], P('batch', 'xsp', 'ysp')
All inputs are finite; a program needn't handle non-finite values.
Results may differ from the reference program's by a relative error of at most 0.00578.
Values are sent between devices in bfloat16 or wider.
A program may use at most 1 GiB of HBM per device.

```python
import jax
import jax.numpy as jnp
from jax import lax

CHANNELS = 64
FILTER_TAPS = 21
LAYERS = 3
GRID_X = 64
GRID_Y = 2048
GRID_Z = 32
HALF_WIDTH = (FILTER_TAPS - 1) // 2


def setup_inputs(seed: int = 0, part: int = 0) -> dict:
    vol_key = jax.random.fold_in(jax.random.key(seed), part)
    key_sign, key_mag, key_mix, key_bias = jax.random.split(jax.random.key(seed + 1), 4)
    volume = jax.random.normal(vol_key, (CHANNELS, GRID_X, GRID_Y, GRID_Z), jnp.float32)
    tap_signs = jnp.where(jax.random.bernoulli(key_sign, 0.5, (LAYERS, 3, FILTER_TAPS)), 1.0, -1.0)
    tap_mags = jax.random.uniform(key_mag, (LAYERS, 3, FILTER_TAPS), jnp.float32, 0.5, 1.0)
    raw_taps = tap_signs * tap_mags
    filter_taps = raw_taps / jnp.sqrt(jnp.sum(raw_taps * raw_taps, axis=-1, keepdims=True))
    mix_weights = jax.random.normal(key_mix, (LAYERS, CHANNELS, CHANNELS), jnp.float32) * CHANNELS ** -0.5
    mix_bias = 0.5 * jax.random.normal(key_bias, (LAYERS, CHANNELS), jnp.float32)
    return {"volume": volume.astype(jnp.bfloat16), "filter_taps": filter_taps, "mix_weights": mix_weights.astype(jnp.bfloat16), "mix_bias": mix_bias}


def line_filter(channel_vol, tap_row, dim_index):
    extent = channel_vol.shape[dim_index]
    pad_cfg = [(0, 0), (0, 0), (0, 0)]
    pad_cfg[dim_index] = (HALF_WIDTH, HALF_WIDTH)
    padded = jnp.pad(channel_vol.astype(jnp.float32), pad_cfg)
    tap_vals = tap_row.astype(jnp.bfloat16).astype(jnp.float32)
    accum_sum = jnp.zeros(channel_vol.shape, jnp.float32)
    for tap_pos in range(FILTER_TAPS):
        accum_sum = accum_sum + tap_vals[tap_pos] * lax.slice_in_dim(padded, tap_pos, tap_pos + extent, axis=dim_index)
    return accum_sum.astype(jnp.bfloat16)


def reference(volume, filter_taps, mix_weights, mix_bias):
    def layer_step(current, params):
        tap_set, mix_mat, bias_vec = params

        def filter_channel(channel_vol):
            x_filtered = line_filter(channel_vol, tap_set[0], 0)
            xy_filtered = line_filter(x_filtered, tap_set[1], 1)
            return line_filter(xy_filtered, tap_set[2], 2)

        smooth = lax.map(filter_channel, current)
        mix_f32 = mix_mat.astype(jnp.float32)

        def mix_plane(pair):
            plane_u, plane_v = pair
            pre_act = jnp.einsum("cd,cyz->dyz", mix_f32, plane_u.astype(jnp.float32)) + bias_vec[:, None, None]
            return (plane_v.astype(jnp.float32) + jax.nn.gelu(pre_act, approximate=True)).astype(jnp.bfloat16)

        planes = lax.map(mix_plane, (jnp.moveaxis(smooth, 1, 0), jnp.moveaxis(current, 1, 0)))
        return jnp.moveaxis(planes, 0, 1), None

    result, _ = lax.scan(layer_step, volume, (filter_taps, mix_weights, mix_bias))
    return result
```

```python
import functools

import jax
import jax.numpy as jnp
from jax import lax
from jax.experimental import pallas as pl
from jax.experimental.pallas import tpu as pltpu
from jax.sharding import PartitionSpec as P

PARTS_AXIS = "batch"
COL_AXIS = "ysp"
ROW_AXIS = "xsp"
H = 10
TAPS = 2 * H + 1
LAYERS = 3
C = 64
BX = 32
BY = 32
BZ = 32
ZL = 16
LANES = 128
CH = 8
NCH = BX // CH
WIN = CH + 2 * H
XS = BX + H
YS = BY + 2 * H
F32 = jnp.float32
BF16 = jnp.bfloat16


def band_times_eye(tap, rows, cols, inner, shift):
    i = lax.broadcasted_iota(jnp.int32, (rows, cols), 0)
    j = lax.broadcasted_iota(jnp.int32, (rows, cols), 1)
    t = j // inner - i // inner + shift
    acc = jnp.zeros((rows, cols), F32)
    for n in range(TAPS):
        acc = jnp.where(t == n, tap(n), acc)
    return jnp.where(i % inner == j % inner, acc, 0.0).astype(BF16)


def kernel(y_count, vol, taps, wmat, bias, out, stage, vbuf, ubuf, tx, ty, tz, w4, in_sem, out_sem, ysend, yrecv, xsend, xrecv):
    xi = lax.axis_index(ROW_AXIS)
    yi = lax.axis_index(COL_AXIS)
    own = xi * H
    has_left = yi > 0
    has_right = yi < y_count - 1
    left = lax.rem(yi + y_count - 1, y_count)
    right = lax.rem(yi + 1, y_count)

    def x_of(k):
        return jnp.where(xi == 0, CH * k, BX - CH - CH * k)

    def load(k):
        x0 = x_of(k)
        return pltpu.make_async_copy(vol.at[pl.ds(x0, CH)], stage.at[k], in_sem.at[k])

    for k in range(NCH):
        load(k).start()

    barrier = pltpu.get_barrier_semaphore()
    pl.semaphore_signal(barrier, inc=1, device_id={COL_AXIS: left})
    pl.semaphore_signal(barrier, inc=1, device_id={COL_AXIS: right})
    pl.semaphore_signal(barrier, inc=1, device_id={ROW_AXIS: 1 - xi})

    def y_copy(l, k, side):
        xs = pl.ds(x_of(k), CH)
        src = ubuf.at[l, xs, pl.ds(H, H)] if side == 0 else ubuf.at[l, xs, pl.ds(BY, H)]
        dst = ubuf.at[l, xs, pl.ds(H + BY, H)] if side == 0 else ubuf.at[l, xs, pl.ds(0, H)]
        return pltpu.make_async_remote_copy(
            src_ref=src, dst_ref=dst, send_sem=ysend.at[l, k, side], recv_sem=yrecv.at[l, k, side],
            device_id={COL_AXIS: left if side == 0 else right})

    def x_copy(l):
        src = jnp.where(xi == 0, BX - H, H)
        dst = jnp.where(xi == 0, 0, BX)
        return pltpu.make_async_remote_copy(
            src_ref=vbuf.at[l, pl.ds(src, H)], dst_ref=vbuf.at[l, pl.ds(dst, H)],
            send_sem=xsend.at[l], recv_sem=xrecv.at[l], device_id={ROW_AXIS: 1 - xi})

    def x_pass(l, k):
        x0 = x_of(k)
        slot = own + x0
        w0 = jnp.clip(slot - H, 0, XS - WIN)
        tx[...] = band_times_eye(lambda n: taps[l * 3, n], CH * ZL, WIN * ZL, ZL, w0 - slot + H)

        def body(j, carry):
            y0 = j * 4
            cols = [vbuf[l, pl.ds(w0, WIN), y0 + i].reshape(WIN * ZL, LANES) for i in range(4)]
            r = jnp.dot(tx[...], jnp.concatenate(cols, axis=1), preferred_element_type=F32).astype(BF16)
            for i in range(4):
                ubuf[l, pl.ds(x0, CH), H + y0 + i] = r[:, LANES * i:LANES * (i + 1)].reshape(CH, ZL, LANES)
            return carry

        lax.fori_loop(0, BY // 4, body, 0)

        @pl.when(has_left)
        def _():
            y_copy(l, k, 0).start()

        @pl.when(has_right)
        def _():
            y_copy(l, k, 1).start()

    def layer_mats(l):
        ty[...] = band_times_eye(lambda n: taps[l * 3 + 1, n], CH * ZL, WIN * ZL, ZL, 0)
        i = lax.broadcasted_iota(jnp.int32, (8 * BZ, 8 * BZ), 0)
        j = lax.broadcasted_iota(jnp.int32, (8 * BZ, 8 * BZ), 1)
        t = j - i + H
        acc = jnp.zeros((8 * BZ, 8 * BZ), F32)
        for n in range(TAPS):
            acc = jnp.where(t == n, taps[l * 3 + 2, n], acc)
        tz[...] = jnp.where(i // BZ == j // BZ, acc, 0.0).astype(BF16)
        w = wmat[l].astype(F32)
        w = jnp.concatenate([w, w], axis=1)
        w = jnp.concatenate([w, w], axis=1)
        w = jnp.concatenate([w, w, w, w], axis=0)
        i = lax.broadcasted_iota(jnp.int32, (4 * C, 4 * C), 0) // C
        j = lax.broadcasted_iota(jnp.int32, (4 * C, 4 * C), 1) // C
        keep = (i // 2 == j % 2) & (i % 2 == j // 2)
        w4[...] = jnp.where(keep, w, 0.0).astype(BF16)

    def y_pass(l, k):
        @pl.when(has_left)
        def _():
            y_copy(l, k, 1).wait_recv()

        @pl.when(has_right)
        def _():
            y_copy(l, k, 0).wait_recv()

        x0 = x_of(k)
        b = bias[pl.ds(l, 1), :]
        b = jnp.concatenate([b, b], axis=1)
        b = jnp.concatenate([b, b], axis=1)
        nxt = jnp.minimum(l + 1, LAYERS - 1)

        def body(it, carry):
            xq = x0 + 4 * (it // 4)
            y0 = pl.multiple_of(8 * (it % 4), 8)
            cols = [ubuf[l, xq + i, pl.ds(y0, WIN)].reshape(WIN * ZL, LANES) for i in range(4)]
            r = jnp.dot(ty[...], jnp.concatenate(cols, axis=1), preferred_element_type=F32).astype(BF16)
            zs = []
            for i in range(4):
                u = r[:, LANES * i:LANES * (i + 1)].reshape(4, 2, ZL, LANES)
                ya, yb = u[:, 0], u[:, 1]
                lo = jnp.concatenate([ya[:, :, :C], yb[:, :, :C]], axis=2)
                hi = jnp.concatenate([ya[:, :, C:], yb[:, :, C:]], axis=2)
                zs.append(jnp.concatenate([lo, hi], axis=1).reshape(4 * BZ, LANES))
            dz = jnp.concatenate([jnp.concatenate([zs[0], zs[1]], axis=0), jnp.concatenate([zs[2], zs[3]], axis=0)], axis=1)
            s = jnp.dot(tz[...], dz, preferred_element_type=F32).astype(BF16)
            lhs = []
            for h in range(2):
                sh = s[:, LANES * h:LANES * (h + 1)].reshape(8, 2, ZL, LANES)
                lhs.append(jnp.concatenate([sh[:, 0], sh[:, 1]], axis=2).reshape(8 * ZL, 2 * LANES))
            m = jnp.dot(jnp.concatenate(lhs, axis=0), w4[...], preferred_element_type=F32) + b
            m = jax.nn.gelu(m, approximate=True)
            for i in range(4):
                mi = m[64 * i:64 * (i + 1)].reshape(4, 1, ZL, 2 * LANES)
                mi = jnp.concatenate([mi[..., :LANES], mi[..., LANES:]], axis=1).reshape(8, ZL, LANES)
                old = vbuf[l, own + xq + i, pl.ds(y0, 8)].astype(F32)
                vbuf[nxt, own + xq + i, pl.ds(y0, 8)] = (old + mi).astype(BF16)
            return carry

        lax.fori_loop(0, 8, body, 0)

    def zero_planes(l, carry):
        vbuf[l, pl.ds(own + x_of(NCH - 1), CH)] = jnp.zeros((CH, BY, ZL, LANES), BF16)
        return carry

    lax.fori_loop(1, LAYERS, zero_planes, 0)

    def zero_halo(y0):
        def body(n, carry):
            ubuf[n // BX, n % BX, pl.ds(y0, H)] = jnp.zeros((H, ZL, LANES), BF16)
            return carry

        lax.fori_loop(0, LAYERS * BX, body, 0)

    def pack(k, carry):
        load(k).wait()
        x0 = x_of(k)

        def body(p, c):
            s = stage[k, p]
            vbuf[0, own + x0 + p] = jnp.concatenate([s[:, :ZL], s[:, ZL:]], axis=2)
            return c

        lax.fori_loop(0, CH, body, 0)
        return carry

    lax.fori_loop(0, NCH, pack, 0)
    pl.semaphore_wait(barrier, 3)
    x_copy(0).start()
    x_pass(0, 0)

    @pl.when(jnp.logical_not(has_left))
    def _():
        zero_halo(0)

    @pl.when(jnp.logical_not(has_right))
    def _():
        zero_halo(H + BY)

    def layer(l, carry):
        def xs(k, c):
            @pl.when(k == 2)
            def _():
                x_copy(l).wait()

            x_pass(l, k)
            return c

        lax.fori_loop(1, NCH, xs, 0)
        layer_mats(l)

        def ys(k, c):
            @pl.when((k == NCH - 1) & (l < LAYERS - 1))
            def _():
                x_pass(l + 1, 0)

            y_pass(l, k)

            @pl.when(l == LAYERS - 1)
            def _():
                store(k).start()

            return c

        lax.fori_loop(0, NCH, ys, 0)

        @pl.when(l < LAYERS - 1)
        def _():
            x_copy(l + 1).start()

        return carry

    def store(k):
        x0 = x_of(k)
        return pltpu.make_async_copy(vbuf.at[LAYERS - 1, pl.ds(own + x0, CH)], out.at[pl.ds(x0, CH)], out_sem.at[k])

    lax.fori_loop(0, LAYERS, layer, 0)

    def finish(n, carry):
        l, k = n // NCH, n % NCH

        @pl.when(has_left)
        def _():
            y_copy(l, k, 0).wait_send()

        @pl.when(has_right)
        def _():
            y_copy(l, k, 1).wait_send()

        return carry

    lax.fori_loop(0, LAYERS * NCH, finish, 0)
    for k in range(NCH):
        store(k).wait()


def unpack_kernel(src, dst):
    s = src[...]
    dst[:, :, :ZL, :] = s[:, :, :, :C]
    dst[:, :, ZL:, :] = s[:, :, :, C:]


def solution(mesh):
    y_count = mesh.shape[COL_AXIS]
    vol_spec = P(PARTS_AXIS, ROW_AXIS, COL_AXIS, None)
    any_spec = pl.BlockSpec(memory_space=pl.ANY)
    vmem_spec = pl.BlockSpec(memory_space=pltpu.VMEM)

    def local_layers(volume, filter_taps, mix_weights, mix_bias):
        vol = jnp.transpose(volume, (1, 2, 3, 0))
        taps = filter_taps.reshape(LAYERS * 3, TAPS)
        packed = pl.pallas_call(
            functools.partial(kernel, y_count),
            out_shape=jax.ShapeDtypeStruct((BX, BY, ZL, LANES), BF16),
            in_specs=[any_spec, pl.BlockSpec(memory_space=pltpu.SMEM), vmem_spec, vmem_spec],
            out_specs=any_spec,
            scratch_shapes=[
                pltpu.VMEM((NCH, CH, BY, BZ, C), BF16),
                pltpu.VMEM((LAYERS, XS, BY, ZL, LANES), BF16),
                pltpu.VMEM((LAYERS, BX, YS, ZL, LANES), BF16),
                pltpu.VMEM((CH * ZL, WIN * ZL), BF16),
                pltpu.VMEM((CH * ZL, WIN * ZL), BF16),
                pltpu.VMEM((8 * BZ, 8 * BZ), BF16),
                pltpu.VMEM((4 * C, 4 * C), BF16),
                pltpu.SemaphoreType.DMA((NCH,)),
                pltpu.SemaphoreType.DMA((NCH,)),
                pltpu.SemaphoreType.DMA((LAYERS, NCH, 2)),
                pltpu.SemaphoreType.DMA((LAYERS, NCH, 2)),
                pltpu.SemaphoreType.DMA((LAYERS,)),
                pltpu.SemaphoreType.DMA((LAYERS,)),
            ],
            compiler_params=pltpu.CompilerParams(collective_id=0, has_side_effects=True, vmem_limit_bytes=60 * 2**20),
        )(vol, taps, mix_weights, mix_bias)
        result = pl.pallas_call(
            unpack_kernel,
            grid=(8,),
            out_shape=jax.ShapeDtypeStruct((BX, BY, BZ, C), BF16),
            in_specs=[pl.BlockSpec((BX // 8, BY, ZL, LANES), lambda i: (i, 0, 0, 0))],
            out_specs=pl.BlockSpec((BX // 8, BY, BZ, C), lambda i: (i, 0, 0, 0)),
        )(packed)
        return jnp.transpose(result, (3, 0, 1, 2))

    return jax.shard_map(local_layers, mesh=mesh, in_specs=(vol_spec, P(), P(), P()), out_specs=vol_spec, check_vma=False)
```

```python
import functools

import jax
import jax.numpy as jnp
from jax import lax
from jax.experimental import pallas as pl
from jax.experimental.pallas import tpu as pltpu
from jax.sharding import PartitionSpec as P

PARTS_AXIS = "batch"
COL_AXIS = "ysp"
ROW_AXIS = "xsp"
H = 10
TAPS = 2 * H + 1
LAYERS = 3
C = 64
BX = 32
BY = 32
BZ = 32
ZL = 16
LANES = 128
CH = 8
NCH = BX // CH
QUAD = 4
NQ = BX // QUAD
WIN = CH + 2 * H
XS = BX + H
YS = BY + 2 * H
SEGS = ((0, H), (BY - H, H), (H, BY - 2 * H))
F32 = jnp.float32
BF16 = jnp.bfloat16


def band_times_eye(tap, rows, cols, inner, shift):
    i = lax.broadcasted_iota(jnp.int32, (rows, cols), 0)
    j = lax.broadcasted_iota(jnp.int32, (rows, cols), 1)
    t = j // inner - i // inner + shift
    acc = jnp.zeros((rows, cols), F32)
    for n in range(TAPS):
        acc = jnp.where(t == n, tap(n), acc)
    return jnp.where(i % inner == j % inner, acc, 0.0).astype(BF16)


def kernel(y_count, vol, taps, wmat, bias, out, stage, vbuf, ubuf, tx, ty, tz, w4, in_sem, out_sem, ysend, yrecv, xsend, xrecv):
    xi = lax.axis_index(ROW_AXIS)
    yi = lax.axis_index(COL_AXIS)
    own = xi * H
    has_left = yi > 0
    has_right = yi < y_count - 1
    left = lax.rem(yi + y_count - 1, y_count)
    right = lax.rem(yi + 1, y_count)

    def x_of(k):
        return jnp.where(xi == 0, CH * k, BX - CH - CH * k)

    def xq_of(q):
        return jnp.where(xi == 0, QUAD * q, BX - QUAD - QUAD * q)

    def load(k, seg):
        ys = pl.ds(*SEGS[seg])
        return pltpu.make_async_copy(vol.at[pl.ds(x_of(k), CH), ys], stage.at[k, :, ys], in_sem.at[k, seg])

    for seg in range(2):
        for k in range(NCH - 1):
            load(k, seg).start()
    load(NCH - 1, 0).start()
    load(NCH - 1, 1).start()
    for k in range(NCH):
        load(k, 2).start()

    barrier = pltpu.get_barrier_semaphore()
    pl.semaphore_signal(barrier, inc=1, device_id={COL_AXIS: left})
    pl.semaphore_signal(barrier, inc=1, device_id={COL_AXIS: right})
    pl.semaphore_signal(barrier, inc=1, device_id={ROW_AXIS: 1 - xi})

    def y_copy(l, q, side):
        xs = pl.ds(xq_of(q), QUAD)
        src = ubuf.at[l, xs, pl.ds(H, H)] if side == 0 else ubuf.at[l, xs, pl.ds(BY, H)]
        dst = ubuf.at[l, xs, pl.ds(H + BY, H)] if side == 0 else ubuf.at[l, xs, pl.ds(0, H)]
        return pltpu.make_async_remote_copy(
            src_ref=src, dst_ref=dst, send_sem=ysend.at[l, q, side], recv_sem=yrecv.at[l, q, side],
            device_id={COL_AXIS: left if side == 0 else right})

    def x_copy(l):
        src = jnp.where(xi == 0, BX - H, H)
        dst = jnp.where(xi == 0, 0, BX)
        return pltpu.make_async_remote_copy(
            src_ref=vbuf.at[l, pl.ds(src, H)], dst_ref=vbuf.at[l, pl.ds(dst, H)],
            send_sem=xsend.at[l], recv_sem=xrecv.at[l], device_id={ROW_AXIS: 1 - xi})

    def window(k):
        slot = own + x_of(k)
        return jnp.clip(slot - H, 0, XS - WIN), slot

    def x_mat(l, k):
        with jax.named_scope("xmat"):
            w0, slot = window(k)
            tx[...] = band_times_eye(lambda n: taps[l, 0, n], CH * ZL, WIN * ZL, ZL, w0 - slot + H)

    def x_seg(l, k, seg):
        with jax.named_scope("xseg"):
            w0, _ = window(k)
            x0 = x_of(k)
            first, count = SEGS[seg]
            cols = [vbuf[l, pl.ds(w0, WIN), first + i].reshape(WIN * ZL, LANES) for i in range(count)]
            r = jnp.dot(tx[...], jnp.concatenate(cols, axis=1), preferred_element_type=F32).astype(BF16)
            for i in range(count):
                ubuf[l, pl.ds(x0, CH), H + first + i] = r[:, LANES * i:LANES * (i + 1)].reshape(CH, ZL, LANES)

    def y_send(l, k, side):
        @pl.when(has_left if side == 0 else has_right)
        def _():
            for j in range(CH // QUAD):
                y_copy(l, k * (CH // QUAD) + j, side).start()

    def x_pass(l, k):
        x_mat(l, k)
        x_seg(l, k, 0)
        y_send(l, k, 0)
        x_seg(l, k, 1)
        y_send(l, k, 1)
        x_seg(l, k, 2)

    def layer_mats(l):
        ty[...] = band_times_eye(lambda n: taps[l, 1, n], CH * ZL, WIN * ZL, ZL, 0)
        i = lax.broadcasted_iota(jnp.int32, (8 * BZ, 8 * BZ), 0)
        j = lax.broadcasted_iota(jnp.int32, (8 * BZ, 8 * BZ), 1)
        t = j - i + H
        acc = jnp.zeros((8 * BZ, 8 * BZ), F32)
        for n in range(TAPS):
            acc = jnp.where(t == n, taps[l, 2, n], acc)
        tz[...] = jnp.where(i // BZ == j // BZ, acc, 0.0).astype(BF16)
        w = wmat[l].astype(F32)
        w = jnp.concatenate([w, w], axis=1)
        w = jnp.concatenate([w, w], axis=1)
        w = jnp.concatenate([w, w, w, w], axis=0)
        i = lax.broadcasted_iota(jnp.int32, (4 * C, 4 * C), 0) // C
        j = lax.broadcasted_iota(jnp.int32, (4 * C, 4 * C), 1) // C
        keep = (i // 2 == j % 2) & (i % 2 == j // 2)
        w4[...] = jnp.where(keep, w, 0.0).astype(BF16)

    def y_quad(l, q):
        with jax.named_scope("ywait"):
            @pl.when(has_left)
            def _():
                y_copy(l, q, 1).wait_recv()

            @pl.when(has_right)
            def _():
                y_copy(l, q, 0).wait_recv()

        with jax.named_scope("yquad"):
            xq = xq_of(q)
            b = bias[pl.ds(l, 1), :]
            b = jnp.concatenate([b, b], axis=1)
            b = jnp.concatenate([b, b], axis=1)
            nxt = jnp.minimum(l + 1, LAYERS - 1)
            rs, ss = [], []
            for g in range(BY // 8):
                cols = [ubuf[l, xq + i, pl.ds(8 * g, WIN)].reshape(WIN * ZL, LANES) for i in range(QUAD)]
                rs.append(jnp.dot(ty[...], jnp.concatenate(cols, axis=1), preferred_element_type=F32).astype(BF16))
            for g in range(BY // 8):
                zs = []
                for i in range(QUAD):
                    u = rs[g][:, LANES * i:LANES * (i + 1)].reshape(4, 2, ZL, LANES)
                    ya, yb = u[:, 0], u[:, 1]
                    lo = jnp.concatenate([ya[:, :, :C], yb[:, :, :C]], axis=2)
                    hi = jnp.concatenate([ya[:, :, C:], yb[:, :, C:]], axis=2)
                    zs.append(jnp.concatenate([lo, hi], axis=1).reshape(4 * BZ, LANES))
                dz = jnp.concatenate([jnp.concatenate(zs[:2], axis=0), jnp.concatenate(zs[2:], axis=0)], axis=1)
                ss.append(jnp.dot(tz[...], dz, preferred_element_type=F32).astype(BF16))
            for g in range(BY // 8):
                lhs = []
                for h in range(2):
                    sh = ss[g][:, LANES * h:LANES * (h + 1)].reshape(8, 2, ZL, LANES)
                    lhs.append(jnp.concatenate([sh[:, 0], sh[:, 1]], axis=2).reshape(8 * ZL, 2 * LANES))
                m = jnp.dot(jnp.concatenate(lhs, axis=0), w4[...], preferred_element_type=F32) + b
                m = jax.nn.gelu(m, approximate=True)
                for i in range(QUAD):
                    mi = m[64 * i:64 * (i + 1)].reshape(4, 1, ZL, 2 * LANES)
                    mi = jnp.concatenate([mi[..., :LANES], mi[..., LANES:]], axis=1).reshape(8, ZL, LANES)
                    old = vbuf[l, own + xq + i, pl.ds(8 * g, 8)].astype(F32)
                    vbuf[nxt, own + xq + i, pl.ds(8 * g, 8)] = (old + mi).astype(BF16)

    def zero_planes(l):
        vbuf[l, pl.ds(own + x_of(NCH - 1), CH)] = jnp.zeros((CH, BY, ZL, LANES), BF16)

    def zero_halo(y0):
        def body(n, carry):
            ubuf[n // BX, n % BX, pl.ds(y0, H)] = jnp.zeros((H, ZL, LANES), BF16)
            return carry

        lax.fori_loop(0, LAYERS * BX, body, 0)

    def pack(k, seg):
        with jax.named_scope("pack"):
            load(k, seg).wait()
            x0 = x_of(k)
            ys = pl.ds(*SEGS[seg])

            def body(p, c):
                s = stage[k, p, ys]
                vbuf[0, own + x0 + p, ys] = jnp.concatenate([s[:, :ZL], s[:, ZL:]], axis=2)
                return c

            lax.fori_loop(0, CH, body, 0)

    def pack_all(seg, n):
        def body(k, c):
            pack(k, seg)
            return c

        lax.fori_loop(0, n, body, 0)

    with jax.named_scope("zero0"):
        zero_planes(0)
    x_mat(0, 0)
    pack_all(0, NCH - 1)
    x_seg(0, 0, 0)
    pl.semaphore_wait(barrier, 3)
    y_send(0, 0, 0)
    pack_all(1, NCH - 1)
    x_seg(0, 0, 1)
    y_send(0, 0, 1)
    pack(NCH - 1, 0)
    pack(NCH - 1, 1)
    pack_all(2, NCH)
    x_copy(0).start()
    x_seg(0, 0, 2)
    for l in range(1, LAYERS):
        zero_planes(l)

    @pl.when(jnp.logical_not(has_left))
    def _():
        zero_halo(0)

    @pl.when(jnp.logical_not(has_right))
    def _():
        zero_halo(H + BY)

    def layer(l, carry):
        def xs(k, c):
            @pl.when(k == 2)
            def _():
                with jax.named_scope("xwait"):
                    x_copy(l).wait()

            x_pass(l, k)
            return c

        lax.fori_loop(1, NCH, xs, 0)
        with jax.named_scope("mats"):
            layer_mats(l)

        def ys(q, c):
            @pl.when((q == NQ - CH // QUAD) & (l < LAYERS - 1))
            def _():
                x_pass(l + 1, 0)

            y_quad(l, q)

            @pl.when(l == LAYERS - 1)
            def _():
                store(q).start()

            return c

        lax.fori_loop(0, NQ, ys, 0)

        @pl.when(l < LAYERS - 1)
        def _():
            x_copy(l + 1).start()

        return carry

    def store(q):
        xs = xq_of(q)
        return pltpu.make_async_copy(vbuf.at[LAYERS - 1, pl.ds(own + xs, QUAD)], out.at[pl.ds(xs, QUAD)], out_sem.at[q])

    lax.fori_loop(0, LAYERS, layer, 0)

    def finish(n, carry):
        l, q = n // NQ, n % NQ

        @pl.when(has_left)
        def _():
            y_copy(l, q, 0).wait_send()

        @pl.when(has_right)
        def _():
            y_copy(l, q, 1).wait_send()

        return carry

    with jax.named_scope("finish"):
        lax.fori_loop(0, LAYERS * NQ, finish, 0)
        for q in range(NQ):
            store(q).wait()


def unpack_kernel(src, dst):
    s = src[...]
    dst[:, :, :ZL, :] = s[:, :, :, :C]
    dst[:, :, ZL:, :] = s[:, :, :, C:]


def solution(mesh):
    y_count = mesh.shape[COL_AXIS]
    vol_spec = P(PARTS_AXIS, ROW_AXIS, COL_AXIS, None)
    any_spec = pl.BlockSpec(memory_space=pl.ANY)
    vmem_spec = pl.BlockSpec(memory_space=pltpu.VMEM)

    def local_layers(volume, filter_taps, mix_weights, mix_bias):
        vol = jnp.transpose(volume, (1, 2, 3, 0))
        packed = pl.pallas_call(
            functools.partial(kernel, y_count),
            out_shape=jax.ShapeDtypeStruct((BX, BY, ZL, LANES), BF16),
            in_specs=[any_spec, pl.BlockSpec(memory_space=pltpu.SMEM), vmem_spec, vmem_spec],
            out_specs=any_spec,
            scratch_shapes=[
                pltpu.VMEM((NCH, CH, BY, BZ, C), BF16),
                pltpu.VMEM((LAYERS, XS, BY, ZL, LANES), BF16),
                pltpu.VMEM((LAYERS, BX, YS, ZL, LANES), BF16),
                pltpu.VMEM((CH * ZL, WIN * ZL), BF16),
                pltpu.VMEM((CH * ZL, WIN * ZL), BF16),
                pltpu.VMEM((8 * BZ, 8 * BZ), BF16),
                pltpu.VMEM((4 * C, 4 * C), BF16),
                pltpu.SemaphoreType.DMA((NCH, 3)),
                pltpu.SemaphoreType.DMA((NQ,)),
                pltpu.SemaphoreType.DMA((LAYERS, NQ, 2)),
                pltpu.SemaphoreType.DMA((LAYERS, NQ, 2)),
                pltpu.SemaphoreType.DMA((LAYERS,)),
                pltpu.SemaphoreType.DMA((LAYERS,)),
            ],
            compiler_params=pltpu.CompilerParams(collective_id=0, has_side_effects=True, vmem_limit_bytes=60 * 2**20),
        )(vol, filter_taps, mix_weights, mix_bias)
        result = pl.pallas_call(
            unpack_kernel,
            grid=(8,),
            out_shape=jax.ShapeDtypeStruct((BX, BY, BZ, C), BF16),
            in_specs=[pl.BlockSpec((BX // 8, BY, ZL, LANES), lambda i: (i, 0, 0, 0))],
            out_specs=pl.BlockSpec((BX // 8, BY, BZ, C), lambda i: (i, 0, 0, 0)),
        )(packed)
        return jnp.transpose(result, (3, 0, 1, 2))

    return jax.shard_map(local_layers, mesh=mesh, in_specs=(vol_spec, P(), P(), P()), out_specs=vol_spec, check_vma=False)
```

```python
import functools

import jax
import jax.numpy as jnp
from jax import lax
from jax.experimental import pallas as pl
from jax.experimental.pallas import tpu as pltpu
from jax.sharding import PartitionSpec as P

PARTS_AXIS = "batch"
COL_AXIS = "ysp"
ROW_AXIS = "xsp"
H = 10
TAPS = 2 * H + 1
LAYERS = 3
C = 64
BX = 32
BY = 32
BZ = 32
ZL = 16
LANES = 128
CH = 8
NCH = BX // CH
QUAD = 4
NQ = BX // QUAD
PART = 4
WIN = CH + 2 * H
XS = BX + H
YS = BY + 2 * H
SEGS = ((0, H), (BY - H, H), (H, BY - 2 * H))
F32 = jnp.float32
BF16 = jnp.bfloat16


def band_times_eye(tap, rows, cols, inner, shift):
    i = lax.broadcasted_iota(jnp.int32, (rows, cols), 0)
    j = lax.broadcasted_iota(jnp.int32, (rows, cols), 1)
    t = j // inner - i // inner + shift
    acc = jnp.zeros((rows, cols), F32)
    for n in range(TAPS):
        acc = jnp.where(t == n, tap(n), acc)
    return jnp.where(i % inner == j % inner, acc, 0.0).astype(BF16)


def kernel(y_count, vol, taps, wmat, bias, out, stage, vbuf, ubuf, tx, ty, tz, w4, in_sem, out_sem, ysend, yrecv, xsend, xrecv):
    xi = lax.axis_index(ROW_AXIS)
    yi = lax.axis_index(COL_AXIS)
    own = xi * H
    has_left = yi > 0
    has_right = yi < y_count - 1
    left = lax.rem(yi + y_count - 1, y_count)
    right = lax.rem(yi + 1, y_count)

    def x_of(k):
        return jnp.where(xi == 0, CH * k, BX - CH - CH * k)

    def xq_of(q):
        return jnp.where(xi == 0, QUAD * q, BX - QUAD - QUAD * q)

    def load(k, seg):
        ys = pl.ds(*SEGS[seg])
        return pltpu.make_async_copy(vol.at[pl.ds(x_of(k), CH), ys], stage.at[k, :, ys], in_sem.at[k, seg])

    for seg in range(2):
        for k in range(NCH - 1):
            load(k, seg).start()
    load(NCH - 1, 0).start()
    load(NCH - 1, 1).start()
    for k in range(NCH):
        load(k, 2).start()

    barrier = pltpu.get_barrier_semaphore()
    pl.semaphore_signal(barrier, inc=1, device_id={COL_AXIS: left})
    pl.semaphore_signal(barrier, inc=1, device_id={COL_AXIS: right})
    pl.semaphore_signal(barrier, inc=1, device_id={ROW_AXIS: 1 - xi})

    def y_copy(l, q, side):
        xs = pl.ds(xq_of(q), QUAD)
        src = ubuf.at[l, xs, pl.ds(H, H)] if side == 0 else ubuf.at[l, xs, pl.ds(BY, H)]
        dst = ubuf.at[l, xs, pl.ds(H + BY, H)] if side == 0 else ubuf.at[l, xs, pl.ds(0, H)]
        return pltpu.make_async_remote_copy(
            src_ref=src, dst_ref=dst, send_sem=ysend.at[l, q, side], recv_sem=yrecv.at[l, q, side],
            device_id={COL_AXIS: left if side == 0 else right})

    def x_copy(l):
        src = jnp.where(xi == 0, BX - H, H)
        dst = jnp.where(xi == 0, 0, BX)
        return pltpu.make_async_remote_copy(
            src_ref=vbuf.at[l, pl.ds(src, H)], dst_ref=vbuf.at[l, pl.ds(dst, H)],
            send_sem=xsend.at[l], recv_sem=xrecv.at[l], device_id={ROW_AXIS: 1 - xi})

    def window(k):
        slot = own + x_of(k)
        return jnp.clip(slot - H, 0, XS - WIN), slot

    def x_mat(l, k):
        with jax.named_scope("xmat"):
            w0, slot = window(k)
            tx[...] = band_times_eye(lambda n: taps[l, 0, n], CH * ZL, WIN * ZL, ZL, w0 - slot + H)

    def x_seg(l, k, seg):
        with jax.named_scope("xseg"):
            w0, _ = window(k)
            x0 = x_of(k)
            first, count = SEGS[seg]
            cols = [vbuf[l, pl.ds(w0, WIN), first + i].reshape(WIN * ZL, LANES) for i in range(count)]
            r = jnp.dot(tx[...], jnp.concatenate(cols, axis=1), preferred_element_type=F32).astype(BF16)
            for i in range(count):
                ubuf[l, pl.ds(x0, CH), H + first + i] = r[:, LANES * i:LANES * (i + 1)].reshape(CH, ZL, LANES)

    def y_send(l, k, side):
        @pl.when(has_left if side == 0 else has_right)
        def _():
            for j in range(CH // QUAD):
                y_copy(l, k * (CH // QUAD) + j, side).start()

    def x_pass(l, k):
        x_mat(l, k)
        x_seg(l, k, 0)
        y_send(l, k, 0)
        x_seg(l, k, 1)
        y_send(l, k, 1)
        x_seg(l, k, 2)

    def layer_mats(l):
        ty[...] = band_times_eye(lambda n: taps[l, 1, n], CH * ZL, WIN * ZL, ZL, 0)
        i = lax.broadcasted_iota(jnp.int32, (8 * BZ, 8 * BZ), 0)
        j = lax.broadcasted_iota(jnp.int32, (8 * BZ, 8 * BZ), 1)
        t = j - i + H
        acc = jnp.zeros((8 * BZ, 8 * BZ), F32)
        for n in range(TAPS):
            acc = jnp.where(t == n, taps[l, 2, n], acc)
        tz[...] = jnp.where(i // BZ == j // BZ, acc, 0.0).astype(BF16)
        w = wmat[l].astype(F32)
        w = jnp.concatenate([w, w], axis=1)
        w = jnp.concatenate([w, w], axis=1)
        w = jnp.concatenate([w, w, w, w], axis=0)
        i = lax.broadcasted_iota(jnp.int32, (4 * C, 4 * C), 0) // C
        j = lax.broadcasted_iota(jnp.int32, (4 * C, 4 * C), 1) // C
        keep = (i // 2 == j % 2) & (i % 2 == j // 2)
        w4[...] = jnp.where(keep, w, 0.0).astype(BF16)

    def y_quad(l, q):
        with jax.named_scope("ywait"):
            @pl.when(has_left)
            def _():
                y_copy(l, q, 1).wait_recv()

            @pl.when(has_right)
            def _():
                y_copy(l, q, 0).wait_recv()

        with jax.named_scope("yquad"):
            xq = xq_of(q)
            b = bias[pl.ds(l, 1), :]
            b = jnp.concatenate([b, b], axis=1)
            b = jnp.concatenate([b, b], axis=1)
            nxt = jnp.minimum(l + 1, LAYERS - 1)
            rs, ss = [], []
            for g in range(BY // 8):
                cols = [ubuf[l, xq + i, pl.ds(8 * g, WIN)].reshape(WIN * ZL, LANES) for i in range(QUAD)]
                rs.append(jnp.dot(ty[...], jnp.concatenate(cols, axis=1), preferred_element_type=F32).astype(BF16))
            for g in range(BY // 8):
                zs = []
                for i in range(QUAD):
                    u = rs[g][:, LANES * i:LANES * (i + 1)].reshape(4, 2, ZL, LANES)
                    ya, yb = u[:, 0], u[:, 1]
                    lo = jnp.concatenate([ya[:, :, :C], yb[:, :, :C]], axis=2)
                    hi = jnp.concatenate([ya[:, :, C:], yb[:, :, C:]], axis=2)
                    zs.append(jnp.concatenate([lo, hi], axis=1).reshape(4 * BZ, LANES))
                dz = jnp.concatenate([jnp.concatenate(zs[:2], axis=0), jnp.concatenate(zs[2:], axis=0)], axis=1)
                ss.append(jnp.dot(tz[...], dz, preferred_element_type=F32).astype(BF16))
            for g in range(BY // 8):
                lhs = []
                for h in range(2):
                    sh = ss[g][:, LANES * h:LANES * (h + 1)].reshape(8, 2, ZL, LANES)
                    lhs.append(jnp.concatenate([sh[:, 0], sh[:, 1]], axis=2).reshape(8 * ZL, 2 * LANES))
                m = jnp.dot(jnp.concatenate(lhs, axis=0), w4[...], preferred_element_type=F32) + b
                m = jax.nn.gelu(m, approximate=True)
                for i in range(QUAD):
                    mi = m[64 * i:64 * (i + 1)].reshape(4, 1, ZL, 2 * LANES)
                    mi = jnp.concatenate([mi[..., :LANES], mi[..., LANES:]], axis=1).reshape(8, ZL, LANES)
                    old = vbuf[l, own + xq + i, pl.ds(8 * g, 8)].astype(F32)
                    vbuf[nxt, own + xq + i, pl.ds(8 * g, 8)] = (old + mi).astype(BF16)

    def zero_planes(l):
        vbuf[l, pl.ds(own + x_of(NCH - 1), CH)] = jnp.zeros((CH, BY, ZL, LANES), BF16)

    def zero_halo(y0):
        def body(n, carry):
            ubuf[n // BX, n % BX, pl.ds(y0, H)] = jnp.zeros((H, ZL, LANES), BF16)
            return carry

        lax.fori_loop(0, LAYERS * BX, body, 0)

    def pack(k, seg):
        with jax.named_scope("pack"):
            load(k, seg).wait()
            x0 = x_of(k)
            ys = pl.ds(*SEGS[seg])

            def body(p, c):
                s = stage[k, p, ys]
                vbuf[0, own + x0 + p, ys] = jnp.concatenate([s[:, :ZL], s[:, ZL:]], axis=2)
                return c

            lax.fori_loop(0, CH, body, 0, unroll=True)

    def pack_all(seg, n):
        def body(k, c):
            pack(k, seg)
            return c

        lax.fori_loop(0, n, body, 0)

    with jax.named_scope("zero0"):
        zero_planes(0)
    x_mat(0, 0)
    pack_all(0, NCH - 1)
    x_seg(0, 0, 0)
    pl.semaphore_wait(barrier, 3)
    y_send(0, 0, 0)
    pack_all(1, NCH - 1)
    x_seg(0, 0, 1)
    y_send(0, 0, 1)
    pack(NCH - 1, 0)
    pack(NCH - 1, 1)
    pack_all(2, NCH)
    x_copy(0).start()
    x_seg(0, 0, 2)
    for l in range(1, LAYERS):
        zero_planes(l)

    @pl.when(jnp.logical_not(has_left))
    def _():
        zero_halo(0)

    @pl.when(jnp.logical_not(has_right))
    def _():
        zero_halo(H + BY)

    def layer(l, carry):
        def xs(k, c):
            @pl.when(k == 2)
            def _():
                with jax.named_scope("xwait"):
                    x_copy(l).wait()

            x_pass(l, k)
            return c

        lax.fori_loop(1, NCH, xs, 0)
        with jax.named_scope("mats"):
            layer_mats(l)

        def ys(q, c):
            @pl.when((q == NQ - CH // QUAD) & (l < LAYERS - 1))
            def _():
                x_pass(l + 1, 0)

            y_quad(l, q)

            @pl.when(l == LAYERS - 1)
            def _():
                store(q).start()

            return c

        lax.fori_loop(0, NQ, ys, 0)

        @pl.when(l < LAYERS - 1)
        def _():
            x_copy(l + 1).start()

        return carry

    def store(q):
        xs = xq_of(q)
        return pltpu.make_async_copy(vbuf.at[LAYERS - 1, pl.ds(own + xs, QUAD)], out.at[pl.ds(xs, QUAD)], out_sem.at[q])

    lax.fori_loop(0, LAYERS, layer, 0)

    def finish(n, carry):
        l, q = n // NQ, n % NQ

        @pl.when(has_left)
        def _():
            y_copy(l, q, 0).wait_send()

        @pl.when(has_right)
        def _():
            y_copy(l, q, 1).wait_send()

        return carry

    with jax.named_scope("finish"):
        lax.fori_loop(0, LAYERS * NQ, finish, 0)
        for q in range(NQ):
            store(q).wait()


def unpack_kernel(src, dst, got, buf, in_sems, out_sems):
    def read(p):
        xs = pl.ds(p * PART, PART)
        return pltpu.make_async_copy(src.at[xs], got.at[xs], in_sems.at[p])

    def write(p):
        xs = pl.ds(p * PART, PART)
        return pltpu.make_async_copy(buf.at[xs], dst.at[xs], out_sems.at[p])

    for p in range(BX // PART):
        read(p).start()

    def body(p, carry):
        xs = pl.ds(p * PART, PART)
        read(p).wait()
        s = got[xs]
        buf[xs, :, :ZL, :] = s[:, :, :, :C]
        buf[xs, :, ZL:, :] = s[:, :, :, C:]
        write(p).start()
        return carry

    lax.fori_loop(0, BX // PART, body, 0)
    for p in range(BX // PART):
        write(p).wait()


def solution(mesh):
    y_count = mesh.shape[COL_AXIS]
    vol_spec = P(PARTS_AXIS, ROW_AXIS, COL_AXIS, None)
    any_spec = pl.BlockSpec(memory_space=pl.ANY)
    vmem_spec = pl.BlockSpec(memory_space=pltpu.VMEM)

    def local_layers(volume, filter_taps, mix_weights, mix_bias):
        vol = jnp.transpose(volume, (1, 2, 3, 0))
        packed = pl.pallas_call(
            functools.partial(kernel, y_count),
            out_shape=jax.ShapeDtypeStruct((BX, BY, ZL, LANES), BF16),
            in_specs=[any_spec, pl.BlockSpec(memory_space=pltpu.SMEM), vmem_spec, vmem_spec],
            out_specs=any_spec,
            scratch_shapes=[
                pltpu.VMEM((NCH, CH, BY, BZ, C), BF16),
                pltpu.VMEM((LAYERS, XS, BY, ZL, LANES), BF16),
                pltpu.VMEM((LAYERS, BX, YS, ZL, LANES), BF16),
                pltpu.VMEM((CH * ZL, WIN * ZL), BF16),
                pltpu.VMEM((CH * ZL, WIN * ZL), BF16),
                pltpu.VMEM((8 * BZ, 8 * BZ), BF16),
                pltpu.VMEM((4 * C, 4 * C), BF16),
                pltpu.SemaphoreType.DMA((NCH, 3)),
                pltpu.SemaphoreType.DMA((NQ,)),
                pltpu.SemaphoreType.DMA((LAYERS, NQ, 2)),
                pltpu.SemaphoreType.DMA((LAYERS, NQ, 2)),
                pltpu.SemaphoreType.DMA((LAYERS,)),
                pltpu.SemaphoreType.DMA((LAYERS,)),
            ],
            compiler_params=pltpu.CompilerParams(collective_id=0, has_side_effects=True, vmem_limit_bytes=60 * 2**20),
        )(vol, filter_taps, mix_weights, mix_bias)
        result = pl.pallas_call(
            unpack_kernel,
            out_shape=jax.ShapeDtypeStruct((BX, BY, BZ, C), BF16),
            in_specs=[any_spec],
            out_specs=any_spec,
            scratch_shapes=[
                pltpu.VMEM((BX, BY, ZL, LANES), BF16),
                pltpu.VMEM((BX, BY, BZ, C), BF16),
                pltpu.SemaphoreType.DMA((BX // PART,)),
                pltpu.SemaphoreType.DMA((BX // PART,)),
            ],
            compiler_params=pltpu.CompilerParams(vmem_limit_bytes=60 * 2**20),
        )(packed)
        return jnp.transpose(result, (3, 0, 1, 2))

    return jax.shard_map(local_layers, mesh=mesh, in_specs=(vol_spec, P(), P(), P()), out_specs=vol_spec, check_vma=False)
```

```python
import functools

import jax
import jax.numpy as jnp
from jax import lax
from jax.experimental import pallas as pl
from jax.experimental.pallas import tpu as pltpu
from jax.sharding import PartitionSpec as P

PARTS_AXIS = "batch"
COL_AXIS = "ysp"
ROW_AXIS = "xsp"
H = 10
TAPS = 2 * H + 1
LAYERS = 3
C = 64
BX = 32
BY = 32
BZ = 32
ZL = 16
LANES = 128
CH = 8
NCH = BX // CH
QUAD = 4
NQ = BX // QUAD
PART = 4
WIN = CH + 2 * H
HEAD = CH + H
XS = BX + H
YS = BY + 2 * H
SEGS = ((0, H), (BY - H, H), (H, BY - 2 * H))
F32 = jnp.float32
BF16 = jnp.bfloat16


def band_times_eye(tap, rows, cols, inner, shift):
    i = lax.broadcasted_iota(jnp.int32, (rows, cols), 0)
    j = lax.broadcasted_iota(jnp.int32, (rows, cols), 1)
    t = j // inner - i // inner + shift
    acc = jnp.zeros((rows, cols), F32)
    for n in range(TAPS):
        acc = jnp.where(t == n, tap(n), acc)
    return jnp.where(i % inner == j % inner, acc, 0.0).astype(BF16)


def kernel(y_count, vol, taps_hbm, wmat_hbm, bias_hbm, out, stage, vbuf, ubuf, tx, ty, tz, w4, taps, wmat, bias, in_sem, small_sem, out_sem, ysend, yrecv, xsend, xrecv):
    xi = lax.axis_index(ROW_AXIS)
    yi = lax.axis_index(COL_AXIS)
    own = xi * H
    has_left = yi > 0
    has_right = yi < y_count - 1
    left = lax.rem(yi + y_count - 1, y_count)
    right = lax.rem(yi + 1, y_count)

    def x_of(k):
        return jnp.where(xi == 0, CH * k, BX - CH - CH * k)

    def xq_of(q):
        return jnp.where(xi == 0, QUAD * q, BX - QUAD - QUAD * q)

    x_head = jnp.where(xi == 0, 0, BX - HEAD)
    x_rest = jnp.where(xi == 0, HEAD, 0)

    def load(n):
        xs = pl.ds(x_rest, BX - HEAD) if n == 2 else pl.ds(x_head, HEAD)
        ys = pl.ds(0, BY) if n == 2 else pl.ds(*SEGS[min(n, 2)])
        return pltpu.make_async_copy(vol.at[xs, ys], stage.at[xs, ys], in_sem.at[n])

    small = [
        pltpu.make_async_copy(taps_hbm, taps, small_sem.at[0]),
        pltpu.make_async_copy(wmat_hbm, wmat, small_sem.at[1]),
        pltpu.make_async_copy(bias_hbm, bias, small_sem.at[2]),
    ]
    small[0].start()
    for n in range(4):
        load(n).start()
    small[1].start()
    small[2].start()

    barrier = pltpu.get_barrier_semaphore()

    @pl.when(has_left)
    def _():
        pl.semaphore_signal(barrier, inc=1, device_id={COL_AXIS: left})

    @pl.when(has_right)
    def _():
        pl.semaphore_signal(barrier, inc=1, device_id={COL_AXIS: right})

    pl.semaphore_signal(barrier, inc=1, device_id={ROW_AXIS: 1 - xi})
    neighbours = 1 + has_left.astype(jnp.int32) + has_right.astype(jnp.int32)

    def y_copy(l, q, side):
        xs = pl.ds(xq_of(q), QUAD)
        src = ubuf.at[l, xs, pl.ds(H, H)] if side == 0 else ubuf.at[l, xs, pl.ds(BY, H)]
        dst = ubuf.at[l, xs, pl.ds(H + BY, H)] if side == 0 else ubuf.at[l, xs, pl.ds(0, H)]
        return pltpu.make_async_remote_copy(
            src_ref=src, dst_ref=dst, send_sem=ysend.at[side], recv_sem=yrecv.at[l, q],
            device_id={COL_AXIS: left if side == 0 else right})

    def x_copy(l):
        src = jnp.where(xi == 0, BX - H, H)
        dst = jnp.where(xi == 0, 0, BX)
        return pltpu.make_async_remote_copy(
            src_ref=vbuf.at[l, pl.ds(src, H)], dst_ref=vbuf.at[l, pl.ds(dst, H)],
            send_sem=xsend.at[l], recv_sem=xrecv.at[l], device_id={ROW_AXIS: 1 - xi})

    def window(k):
        slot = own + x_of(k)
        return jnp.clip(slot - H, 0, XS - WIN), slot

    def x_mat(l, k):
        with jax.named_scope("xmat"):
            w0, slot = window(k)
            tx[...] = band_times_eye(lambda n: taps[l, 0, n], CH * ZL, WIN * ZL, ZL, w0 - slot + H)

    def x_seg(l, k, seg):
        with jax.named_scope("xseg"):
            w0, _ = window(k)
            x0 = x_of(k)
            first, count = SEGS[seg]
            cols = [vbuf[l, pl.ds(w0, WIN), first + i].reshape(WIN * ZL, LANES) for i in range(count)]
            r = jnp.dot(tx[...], jnp.concatenate(cols, axis=1), preferred_element_type=F32).astype(BF16)
            for i in range(count):
                ubuf[l, pl.ds(x0, CH), H + first + i] = r[:, LANES * i:LANES * (i + 1)].reshape(CH, ZL, LANES)

    def y_send(l, k, side):
        @pl.when(has_left if side == 0 else has_right)
        def _():
            for j in range(CH // QUAD):
                y_copy(l, k * (CH // QUAD) + j, side).start()

    def x_pass(l, k):
        x_mat(l, k)
        x_seg(l, k, 0)
        y_send(l, k, 0)
        x_seg(l, k, 1)
        y_send(l, k, 1)
        x_seg(l, k, 2)

    def layer_mats(l):
        ty[...] = band_times_eye(lambda n: taps[l, 1, n], CH * ZL, WIN * ZL, ZL, 0)
        i = lax.broadcasted_iota(jnp.int32, (8 * BZ, 8 * BZ), 0)
        j = lax.broadcasted_iota(jnp.int32, (8 * BZ, 8 * BZ), 1)
        t = j - i + H
        acc = jnp.zeros((8 * BZ, 8 * BZ), F32)
        for n in range(TAPS):
            acc = jnp.where(t == n, taps[l, 2, n], acc)
        tz[...] = jnp.where(i // BZ == j // BZ, acc, 0.0).astype(BF16)
        w = wmat[l].astype(F32)
        w = jnp.concatenate([w, w], axis=1)
        w = jnp.concatenate([w, w], axis=1)
        w = jnp.concatenate([w, w, w, w], axis=0)
        i = lax.broadcasted_iota(jnp.int32, (4 * C, 4 * C), 0) // C
        j = lax.broadcasted_iota(jnp.int32, (4 * C, 4 * C), 1) // C
        keep = (i // 2 == j % 2) & (i % 2 == j // 2)
        w4[...] = jnp.where(keep, w, 0.0).astype(BF16)

    def y_quad(l, q):
        with jax.named_scope("ywait"):
            both = ubuf.at[l, pl.ds(xq_of(q), QUAD), pl.ds(0, 2 * H)]

            @pl.when(has_left & has_right)
            def _():
                pltpu.make_async_remote_copy(
                    src_ref=both, dst_ref=both, send_sem=ysend.at[0], recv_sem=yrecv.at[l, q],
                    device_id={COL_AXIS: left}).wait_recv()

            @pl.when(jnp.logical_not(has_left & has_right))
            def _():
                y_copy(l, q, 0).wait_recv()

        with jax.named_scope("yquad"):
            xq = xq_of(q)
            b = bias[pl.ds(l, 1), :]
            b = jnp.concatenate([b, b], axis=1)
            b = jnp.concatenate([b, b], axis=1)
            nxt = jnp.minimum(l + 1, LAYERS - 1)
            rs, ss = [], []
            for g in range(BY // 8):
                cols = [ubuf[l, xq + i, pl.ds(8 * g, WIN)].reshape(WIN * ZL, LANES) for i in range(QUAD)]
                rs.append(jnp.dot(ty[...], jnp.concatenate(cols, axis=1), preferred_element_type=F32).astype(BF16))
            for g in range(BY // 8):
                zs = []
                for i in range(QUAD):
                    u = rs[g][:, LANES * i:LANES * (i + 1)].reshape(4, 2, ZL, LANES)
                    ya, yb = u[:, 0], u[:, 1]
                    lo = jnp.concatenate([ya[:, :, :C], yb[:, :, :C]], axis=2)
                    hi = jnp.concatenate([ya[:, :, C:], yb[:, :, C:]], axis=2)
                    zs.append(jnp.concatenate([lo, hi], axis=1).reshape(4 * BZ, LANES))
                dz = jnp.concatenate([jnp.concatenate(zs[:2], axis=0), jnp.concatenate(zs[2:], axis=0)], axis=1)
                ss.append(jnp.dot(tz[...], dz, preferred_element_type=F32).astype(BF16))
            for g in range(BY // 8):
                lhs = []
                for h in range(2):
                    sh = ss[g][:, LANES * h:LANES * (h + 1)].reshape(8, 2, ZL, LANES)
                    lhs.append(jnp.concatenate([sh[:, 0], sh[:, 1]], axis=2).reshape(8 * ZL, 2 * LANES))
                m = jnp.dot(jnp.concatenate(lhs, axis=0), w4[...], preferred_element_type=F32) + b
                m = jax.nn.gelu(m, approximate=True)
                for i in range(QUAD):
                    mi = m[64 * i:64 * (i + 1)].reshape(4, 1, ZL, 2 * LANES)
                    mi = jnp.concatenate([mi[..., :LANES], mi[..., LANES:]], axis=1).reshape(8, ZL, LANES)
                    old = vbuf[l, own + xq + i, pl.ds(8 * g, 8)].astype(F32)
                    vbuf[nxt, own + xq + i, pl.ds(8 * g, 8)] = (old + mi).astype(BF16)

    def zero_planes(l):
        vbuf[l, pl.ds(own + x_of(NCH - 1), CH)] = jnp.zeros((CH, BY, ZL, LANES), BF16)

    def zero_halo(l, y0):
        def body(n, carry):
            ubuf[l, n, pl.ds(y0, H)] = jnp.zeros((H, ZL, LANES), BF16)
            return carry

        lax.fori_loop(0, BX, body, 0)

    def pack(n, x0, count, first, ny):
        with jax.named_scope("pack"):
            ys = pl.ds(first, ny)

            def body(p, c):
                s = stage[x0 + p, ys]
                vbuf[0, own + x0 + p, ys] = jnp.concatenate([s[:, :ZL], s[:, ZL:]], axis=2)
                return c

            lax.fori_loop(0, count, body, 0, unroll=True)

    with jax.named_scope("zero0"):
        for seg in range(2):
            first, ny = SEGS[seg]
            pad = WIN - HEAD
            vbuf[0, pl.ds(own + jnp.where(xi == 0, HEAD, BX - WIN), pad), pl.ds(first, ny)] = jnp.zeros((pad, ny, ZL, LANES), BF16)
    small[0].wait()
    x_mat(0, 0)
    load(0).wait()
    pack(0, x_head, HEAD, *SEGS[0])
    x_seg(0, 0, 0)
    with jax.named_scope("barrier"):
        pl.semaphore_wait(barrier, neighbours)
    y_send(0, 0, 0)
    load(1).wait()
    pack(1, x_head, HEAD, *SEGS[1])
    x_seg(0, 0, 1)
    y_send(0, 0, 1)
    load(2).wait()
    pack(2, x_rest, BX - HEAD, 0, BY)
    x_copy(0).start()
    load(3).wait()
    pack(3, x_head, HEAD, *SEGS[2])
    x_seg(0, 0, 2)
    for l in range(1, LAYERS):
        zero_planes(l)
    small[1].wait()
    small[2].wait()

    def layer(l, carry):
        def xs(k, c):
            @pl.when(k == 2)
            def _():
                with jax.named_scope("xwait"):
                    x_copy(l).wait()

            x_pass(l, k)
            return c

        lax.fori_loop(1, NCH, xs, 0)
        with jax.named_scope("mats"):
            layer_mats(l)

        @pl.when(jnp.logical_not(has_left))
        def _():
            zero_halo(l, 0)

        @pl.when(jnp.logical_not(has_right))
        def _():
            zero_halo(l, H + BY)

        def ys(q, c):
            @pl.when((q == NQ - CH // QUAD) & (l < LAYERS - 1))
            def _():
                x_pass(l + 1, 0)

            y_quad(l, q)

            @pl.when(l == LAYERS - 1)
            def _():
                store(q).start()

            return c

        lax.fori_loop(0, NQ, ys, 0)

        @pl.when(l < LAYERS - 1)
        def _():
            x_copy(l + 1).start()

        return carry

    def store(q):
        xs = xq_of(q)
        return pltpu.make_async_copy(vbuf.at[LAYERS - 1, pl.ds(own + xs, QUAD)], out.at[pl.ds(xs, QUAD)], out_sem)

    lax.fori_loop(0, LAYERS, layer, 0)

    with jax.named_scope("finish"):
        for side in range(2):
            sent = ubuf.at[:, :, pl.ds(0, H)]

            @pl.when(has_left if side == 0 else has_right)
            def _():
                pltpu.make_async_remote_copy(
                    src_ref=sent, dst_ref=sent, send_sem=ysend.at[side], recv_sem=yrecv.at[0, 0],
                    device_id={COL_AXIS: left if side == 0 else right}).wait_send()

        pltpu.make_async_copy(vbuf.at[LAYERS - 1, pl.ds(own, BX)], out, out_sem).wait()


def unpack_kernel(src, dst, got, buf, in_sems, out_sem):
    def read(p):
        xs = pl.ds(p * PART, PART)
        return pltpu.make_async_copy(src.at[xs], got.at[xs], in_sems.at[p])

    def write(p):
        xs = pl.ds(p * PART, PART)
        return pltpu.make_async_copy(buf.at[xs], dst.at[xs], out_sem)

    for p in range(BX // PART):
        read(p).start()

    def body(p, carry):
        xs = pl.ds(p * PART, PART)
        read(p).wait()
        s = got[xs]
        buf[xs, :, :ZL, :] = s[:, :, :, :C]
        buf[xs, :, ZL:, :] = s[:, :, :, C:]
        write(p).start()
        return carry

    lax.fori_loop(0, BX // PART, body, 0)
    pltpu.make_async_copy(buf, dst, out_sem).wait()


def solution(mesh):
    y_count = mesh.shape[COL_AXIS]
    vol_spec = P(PARTS_AXIS, ROW_AXIS, COL_AXIS, None)
    any_spec = pl.BlockSpec(memory_space=pl.ANY)

    def local_layers(volume, filter_taps, mix_weights, mix_bias):
        vol = jnp.transpose(volume, (1, 2, 3, 0))
        packed = pl.pallas_call(
            functools.partial(kernel, y_count),
            out_shape=jax.ShapeDtypeStruct((BX, BY, ZL, LANES), BF16),
            in_specs=[any_spec] * 4,
            out_specs=any_spec,
            scratch_shapes=[
                pltpu.VMEM((BX, BY, BZ, C), BF16),
                pltpu.VMEM((LAYERS, XS, BY, ZL, LANES), BF16),
                pltpu.VMEM((LAYERS, BX, YS, ZL, LANES), BF16),
                pltpu.VMEM((CH * ZL, WIN * ZL), BF16),
                pltpu.VMEM((CH * ZL, WIN * ZL), BF16),
                pltpu.VMEM((8 * BZ, 8 * BZ), BF16),
                pltpu.VMEM((4 * C, 4 * C), BF16),
                pltpu.SMEM((LAYERS, 3, TAPS), F32),
                pltpu.VMEM((LAYERS, C, C), BF16),
                pltpu.VMEM((LAYERS, C), F32),
                pltpu.SemaphoreType.DMA((4,)),
                pltpu.SemaphoreType.DMA((3,)),
                pltpu.SemaphoreType.DMA,
                pltpu.SemaphoreType.DMA((2,)),
                pltpu.SemaphoreType.DMA((LAYERS, NQ)),
                pltpu.SemaphoreType.DMA((LAYERS,)),
                pltpu.SemaphoreType.DMA((LAYERS,)),
            ],
            compiler_params=pltpu.CompilerParams(collective_id=0, has_side_effects=True, vmem_limit_bytes=60 * 2**20),
        )(vol, filter_taps, mix_weights, mix_bias)
        result = pl.pallas_call(
            unpack_kernel,
            out_shape=jax.ShapeDtypeStruct((BX, BY, BZ, C), BF16),
            in_specs=[any_spec],
            out_specs=any_spec,
            scratch_shapes=[
                pltpu.VMEM((BX, BY, ZL, LANES), BF16),
                pltpu.VMEM((BX, BY, BZ, C), BF16),
                pltpu.SemaphoreType.DMA((BX // PART,)),
                pltpu.SemaphoreType.DMA,
            ],
            compiler_params=pltpu.CompilerParams(vmem_limit_bytes=60 * 2**20),
        )(packed)
        return jnp.transpose(result, (3, 0, 1, 2))

    return jax.shard_map(local_layers, mesh=mesh, in_specs=(vol_spec, P(), P(), P()), out_specs=vol_spec, check_vma=False)
```

```python
import functools

import jax
import jax.numpy as jnp
from jax import lax
from jax.experimental import pallas as pl
from jax.experimental.pallas import tpu as pltpu
from jax.sharding import PartitionSpec as P

PARTS_AXIS = "batch"
COL_AXIS = "ysp"
ROW_AXIS = "xsp"
H = 10
TAPS = 2 * H + 1
LAYERS = 3
C = 64
BX = 32
BY = 32
BZ = 32
ZL = 16
LANES = 128
CH = 8
NCH = BX // CH
QUAD = 4
NQ = BX // QUAD
WIN = CH + 2 * H
HEAD = CH + H
XS = BX + H
YS = BY + 2 * H
SEGS = ((BY - H, H), (0, H), (H, BY - 2 * H))
F32 = jnp.float32
BF16 = jnp.bfloat16


def band_times_eye(tap, rows, cols, inner, shift):
    i = lax.broadcasted_iota(jnp.int32, (rows, cols), 0)
    j = lax.broadcasted_iota(jnp.int32, (rows, cols), 1)
    t = j // inner - i // inner + shift
    acc = jnp.zeros((rows, cols), F32)
    for n in range(TAPS):
        acc = jnp.where(t == n, tap(n), acc)
    return jnp.where(i % inner == j % inner, acc, 0.0).astype(BF16)


def y_compute(window_of, old, put, ty, tz, w4, b):
    b = jnp.concatenate([b, b], axis=1)
    b = jnp.concatenate([b, b], axis=1)
    rs, ss = [], []
    for g in range(BY // 8):
        cols = [window_of(i, 8 * g).reshape(WIN * ZL, LANES) for i in range(QUAD)]
        rs.append(jnp.dot(ty[...], jnp.concatenate(cols, axis=1), preferred_element_type=F32).astype(BF16))
    for g in range(BY // 8):
        zs = []
        for i in range(QUAD):
            u = rs[g][:, LANES * i:LANES * (i + 1)].reshape(4, 2, ZL, LANES)
            ya, yb = u[:, 0], u[:, 1]
            lo = jnp.concatenate([ya[:, :, :C], yb[:, :, :C]], axis=2)
            hi = jnp.concatenate([ya[:, :, C:], yb[:, :, C:]], axis=2)
            zs.append(jnp.concatenate([lo, hi], axis=1).reshape(4 * BZ, LANES))
        dz = jnp.concatenate([jnp.concatenate(zs[:2], axis=0), jnp.concatenate(zs[2:], axis=0)], axis=1)
        ss.append(jnp.dot(tz[...], dz, preferred_element_type=F32).astype(BF16))
    for g in range(BY // 8):
        lhs = []
        for h in range(2):
            sh = ss[g][:, LANES * h:LANES * (h + 1)].reshape(8, 2, ZL, LANES)
            lhs.append(jnp.concatenate([sh[:, 0], sh[:, 1]], axis=2).reshape(8 * ZL, 2 * LANES))
        m = jnp.dot(jnp.concatenate(lhs, axis=0), w4[...], preferred_element_type=F32) + b
        m = jax.nn.gelu(m, approximate=True)
        for i in range(QUAD):
            mi = m[64 * i:64 * (i + 1)].reshape(4, 1, ZL, 2 * LANES)
            mi = jnp.concatenate([mi[..., :LANES], mi[..., LANES:]], axis=1).reshape(8, ZL, LANES)
            put(i, 8 * g, (old(i, 8 * g).astype(F32) + mi).astype(BF16))


def kernel(y_count, vol, taps_hbm, wmat_hbm, bias_hbm, out, u_out, ty_out, tz_out, w4_out, stage, vbuf, ubuf, tx, ty, tz, w4, taps, wmat, bias, in_sem, small_sem, out_sem, ysend, yrecv, xsend, xrecv):
    xi = lax.axis_index(ROW_AXIS)
    yi = lax.axis_index(COL_AXIS)
    own = xi * H
    has_left = yi > 0
    has_right = yi < y_count - 1
    left = lax.rem(yi + y_count - 1, y_count)
    right = lax.rem(yi + 1, y_count)

    def x_of(k):
        return jnp.where(xi == 0, CH * k, BX - CH - CH * k)

    def xq_of(q):
        return jnp.where(xi == 0, QUAD * q, BX - QUAD - QUAD * q)

    x_head = jnp.where(xi == 0, 0, BX - HEAD)
    x_rest = jnp.where(xi == 0, HEAD, 0)

    def load(n):
        xs = pl.ds(x_rest, BX - HEAD) if n == 2 else pl.ds(x_head, HEAD)
        ys = pl.ds(0, BY) if n == 2 else pl.ds(*SEGS[min(n, 2)])
        return pltpu.make_async_copy(vol.at[xs, ys], stage.at[xs, ys], in_sem.at[n])

    small = [
        pltpu.make_async_copy(taps_hbm, taps, small_sem.at[0]),
        pltpu.make_async_copy(wmat_hbm, wmat, small_sem.at[1]),
        pltpu.make_async_copy(bias_hbm, bias, small_sem.at[2]),
    ]
    small[0].start()
    for n in range(4):
        load(n).start()
    small[1].start()
    small[2].start()

    barrier = pltpu.get_barrier_semaphore()

    @pl.when(has_left)
    def _():
        pl.semaphore_signal(barrier, inc=1, device_id={COL_AXIS: left})

    @pl.when(has_right)
    def _():
        pl.semaphore_signal(barrier, inc=1, device_id={COL_AXIS: right})

    pl.semaphore_signal(barrier, inc=1, device_id={ROW_AXIS: 1 - xi})
    neighbours = 1 + has_left.astype(jnp.int32) + has_right.astype(jnp.int32)

    def y_copy(l, q, side):
        xs = pl.ds(xq_of(q), QUAD)
        src = ubuf.at[l, xs, pl.ds(H, H)] if side == 0 else ubuf.at[l, xs, pl.ds(BY, H)]
        dst = ubuf.at[l, xs, pl.ds(H + BY, H)] if side == 0 else ubuf.at[l, xs, pl.ds(0, H)]
        return pltpu.make_async_remote_copy(
            src_ref=src, dst_ref=dst, send_sem=ysend.at[side], recv_sem=yrecv.at[l, q],
            device_id={COL_AXIS: left if side == 0 else right})

    def x_copy(l):
        src = jnp.where(xi == 0, BX - H, H)
        dst = jnp.where(xi == 0, 0, BX)
        return pltpu.make_async_remote_copy(
            src_ref=vbuf.at[l, pl.ds(src, H)], dst_ref=vbuf.at[l, pl.ds(dst, H)],
            send_sem=xsend.at[l], recv_sem=xrecv.at[l], device_id={ROW_AXIS: 1 - xi})

    def window(k):
        slot = own + x_of(k)
        return jnp.clip(slot - H, 0, XS - WIN), slot

    def x_mat(l, k):
        with jax.named_scope("xmat"):
            w0, slot = window(k)
            tx[...] = band_times_eye(lambda n: taps[l, 0, n], CH * ZL, WIN * ZL, ZL, w0 - slot + H)

    def x_seg(l, k, seg):
        with jax.named_scope("xseg"):
            w0, _ = window(k)
            x0 = x_of(k)
            first, count = SEGS[seg]
            cols = [vbuf[l, pl.ds(w0, WIN), first + i].reshape(WIN * ZL, LANES) for i in range(count)]
            r = jnp.dot(tx[...], jnp.concatenate(cols, axis=1), preferred_element_type=F32).astype(BF16)
            for i in range(count):
                ubuf[l, pl.ds(x0, CH), H + first + i] = r[:, LANES * i:LANES * (i + 1)].reshape(CH, ZL, LANES)

    def last_copy(side):
        l, q = LAYERS - 1, NQ - 1
        src = ubuf.at[l, pl.ds(xq_of(q), QUAD), pl.ds(H if side == 0 else BY, H)]
        return pltpu.make_async_remote_copy(
            src_ref=src, dst_ref=u_out.at[:, pl.ds(H + BY if side == 0 else 0, H)], send_sem=ysend.at[side], recv_sem=yrecv.at[l, q],
            device_id={COL_AXIS: left if side == 0 else right})

    def y_send(l, k, side):
        goes = has_left if side == 0 else has_right
        for j in range(CH // QUAD):
            q = k * (CH // QUAD) + j
            last = (l == LAYERS - 1) & (q == NQ - 1)

            @pl.when(goes & jnp.logical_not(last))
            def _():
                y_copy(l, q, side).start()

            @pl.when(goes & last)
            def _():
                last_copy(side).start()

    def x_pass(l, k):
        x_mat(l, k)
        x_seg(l, k, 0)
        y_send(l, k, 1)
        x_seg(l, k, 1)
        y_send(l, k, 0)
        x_seg(l, k, 2)

    def layer_mats(l):
        ty[...] = band_times_eye(lambda n: taps[l, 1, n], CH * ZL, WIN * ZL, ZL, 0)
        i = lax.broadcasted_iota(jnp.int32, (8 * BZ, 8 * BZ), 0)
        j = lax.broadcasted_iota(jnp.int32, (8 * BZ, 8 * BZ), 1)
        t = j - i + H
        acc = jnp.zeros((8 * BZ, 8 * BZ), F32)
        for n in range(TAPS):
            acc = jnp.where(t == n, taps[l, 2, n], acc)
        tz[...] = jnp.where(i // BZ == j // BZ, acc, 0.0).astype(BF16)
        w = wmat[l].astype(F32)
        w = jnp.concatenate([w, w], axis=1)
        w = jnp.concatenate([w, w], axis=1)
        w = jnp.concatenate([w, w, w, w], axis=0)
        i = lax.broadcasted_iota(jnp.int32, (4 * C, 4 * C), 0) // C
        j = lax.broadcasted_iota(jnp.int32, (4 * C, 4 * C), 1) // C
        keep = (i // 2 == j % 2) & (i % 2 == j // 2)
        w4[...] = jnp.where(keep, w, 0.0).astype(BF16)

    def y_wait(l, q):
        with jax.named_scope("ywait"):
            both = ubuf.at[l, pl.ds(xq_of(q), QUAD), pl.ds(0, 2 * H)]

            @pl.when(has_left & has_right)
            def _():
                pltpu.make_async_remote_copy(
                    src_ref=both, dst_ref=both, send_sem=ysend.at[0], recv_sem=yrecv.at[l, q],
                    device_id={COL_AXIS: left}).wait_recv()

            @pl.when(jnp.logical_not(has_left & has_right))
            def _():
                y_copy(l, q, 0).wait_recv()

    def y_quad(l, q):
        y_wait(l, q)
        with jax.named_scope("yquad"):
            xq = xq_of(q)
            nxt = jnp.minimum(l + 1, LAYERS - 1)

            def window_of(i, y0):
                return ubuf[l, xq + i, pl.ds(y0, WIN)]

            def old(i, y0):
                return vbuf[l, own + xq + i, pl.ds(y0, 8)]

            def put(i, y0, v):
                vbuf[nxt, own + xq + i, pl.ds(y0, 8)] = v

            y_compute(window_of, old, put, ty, tz, w4, bias[pl.ds(l, 1), :])

    def zero_planes(l):
        vbuf[l, pl.ds(own + x_of(NCH - 1), CH)] = jnp.zeros((CH, BY, ZL, LANES), BF16)

    def zero_halo(l, y0):
        def body(n, carry):
            ubuf[l, n, pl.ds(y0, H)] = jnp.zeros((H, ZL, LANES), BF16)
            return carry

        lax.fori_loop(0, BX, body, 0)

    def pack(n, x0, count, first, ny):
        with jax.named_scope("pack"):
            ys = pl.ds(first, ny)

            def body(p, c):
                s = stage[x0 + p, ys]
                vbuf[0, own + x0 + p, ys] = jnp.concatenate([s[:, :ZL], s[:, ZL:]], axis=2)
                return c

            lax.fori_loop(0, count, body, 0, unroll=True)

    with jax.named_scope("zero0"):
        for seg in range(2):
            first, ny = SEGS[seg]
            pad = WIN - HEAD
            vbuf[0, pl.ds(own + jnp.where(xi == 0, HEAD, BX - WIN), pad), pl.ds(first, ny)] = jnp.zeros((pad, ny, ZL, LANES), BF16)
    small[0].wait()
    x_mat(0, 0)
    load(0).wait()
    pack(0, x_head, HEAD, *SEGS[0])
    x_seg(0, 0, 0)
    with jax.named_scope("barrier"):
        pl.semaphore_wait(barrier, neighbours)
    y_send(0, 0, 1)
    load(1).wait()
    pack(1, x_head, HEAD, *SEGS[1])
    x_seg(0, 0, 1)
    y_send(0, 0, 0)
    load(2).wait()
    pack(2, x_rest, BX - HEAD, 0, BY)
    x_copy(0).start()
    load(3).wait()
    pack(3, x_head, HEAD, *SEGS[2])
    x_seg(0, 0, 2)
    for l in range(1, LAYERS):
        zero_planes(l)
    small[1].wait()
    small[2].wait()

    def layer(l, carry):
        def xs(k, c):
            @pl.when(k == 2)
            def _():
                with jax.named_scope("xwait"):
                    x_copy(l).wait()

            x_pass(l, k)
            return c

        lax.fori_loop(1, NCH, xs, 0)
        with jax.named_scope("mats"):
            layer_mats(l)

        @pl.when(jnp.logical_not(has_left))
        def _():
            zero_halo(l, 0)

        @pl.when(jnp.logical_not(has_right))
        def _():
            zero_halo(l, H + BY)

        @pl.when(l == LAYERS - 1)
        def _():
            store(NQ - 1).start()
            for mat in store_mats:
                mat.start()
            store_u.start()
            for edge, copy in store_edges:
                pl.when(edge)(copy.start)

        def ys(q, c):
            @pl.when((q == NQ - CH // QUAD) & (l < LAYERS - 1))
            def _():
                x_pass(l + 1, 0)

            @pl.when((q < NQ - 1) | (l < LAYERS - 1))
            def _():
                y_quad(l, q)

            @pl.when((q < NQ - 1) & (l == LAYERS - 1))
            def _():
                store(q).start()

            return c

        lax.fori_loop(0, NQ, ys, 0)

        @pl.when(l < LAYERS - 1)
        def _():
            x_copy(l + 1).start()

        return carry

    def store(q):
        xs = xq_of(q)
        return pltpu.make_async_copy(vbuf.at[LAYERS - 1, pl.ds(own + xs, QUAD)], out.at[pl.ds(xs, QUAD)], out_sem)

    store_mats = [pltpu.make_async_copy(m, o, small_sem.at[n]) for n, (m, o) in enumerate(((ty, ty_out), (tz, tz_out), (w4, w4_out)))]
    last_u = ubuf.at[LAYERS - 1, pl.ds(xq_of(NQ - 1), QUAD)]
    store_u = pltpu.make_async_copy(last_u.at[:, pl.ds(H, BY)], u_out.at[:, pl.ds(H, BY)], in_sem.at[0])
    store_edges = [
        (jnp.logical_not(has), pltpu.make_async_copy(last_u.at[:, pl.ds(y0, H)], u_out.at[:, pl.ds(y0, H)], in_sem.at[n]))
        for has, y0, n in ((has_left, 0, 2), (has_right, H + BY, 3))
    ]
    lax.fori_loop(0, LAYERS, layer, 0)
    y_wait(LAYERS - 1, NQ - 1)

    with jax.named_scope("finish"):
        for side in range(2):
            sent = ubuf.at[:, :, pl.ds(0, H)]

            @pl.when(has_left if side == 0 else has_right)
            def _():
                pltpu.make_async_remote_copy(
                    src_ref=sent, dst_ref=sent, send_sem=ysend.at[side], recv_sem=yrecv.at[0, 0],
                    device_id={COL_AXIS: left if side == 0 else right}).wait_send()

        pltpu.make_async_copy(vbuf.at[LAYERS - 1, pl.ds(own, BX)], out, out_sem).wait()
        for edge, copy in store_edges:
            pl.when(edge)(copy.wait)
        for mat in store_mats:
            mat.wait()
        store_u.wait()


def unpack(s):
    r = pltpu.roll(s.reshape(QUAD * BY * ZL, LANES), C, 1).reshape(QUAD, BY, ZL, LANES)
    return s[:, :, :, :C], r[:, :, :, :C]


def last_kernel(src, u_hbm, ty_hbm, tz_hbm, w4_hbm, bias_hbm, dst, got, u, ty, tz, w4, bias, buf, in_sems, mat_sems, out_sem):
    xi = lax.axis_index(ROW_AXIS)

    def planes(q):
        return pl.ds(jnp.where(xi == 0, QUAD * q, BX - QUAD - QUAD * q), QUAD)

    def read(q):
        return pltpu.make_async_copy(src.at[planes(q)], got.at[planes(q)], in_sems.at[q])

    def write(q):
        return pltpu.make_async_copy(buf.at[planes(q)], dst.at[planes(q)], out_sem)

    mats = [
        pltpu.make_async_copy(h, v, mat_sems.at[n])
        for n, (h, v) in enumerate(((u_hbm, u), (ty_hbm, ty), (tz_hbm, tz), (w4_hbm, w4), (bias_hbm, bias)))
    ]
    for q in range(NQ - 1):
        read(q).start()
    for mat in mats:
        mat.start()
    read(NQ - 1).start()

    def body(q, carry):
        read(q).wait()
        buf[planes(q), :, :ZL, :], buf[planes(q), :, ZL:, :] = unpack(got[planes(q)])
        write(q).start()
        return carry

    with jax.named_scope("unpack"):
        lax.fori_loop(0, NQ - 1, body, 0)
    with jax.named_scope("matwait"):
        for mat in mats:
            mat.wait()
        read(NQ - 1).wait()
    xq = jnp.where(xi == 0, BX - QUAD, 0)

    def put(i, y0, v):
        buf[xq + i, pl.ds(y0, 8), :ZL, :] = v[:, :, :C]
        buf[xq + i, pl.ds(y0, 8), ZL:, :] = v[:, :, C:]

    with jax.named_scope("ycomp"):
        y_compute(
            lambda i, y0: u[i, pl.ds(y0, WIN)], lambda i, y0: got[xq + i, pl.ds(y0, 8)], put,
            ty, tz, w4, bias[pl.ds(LAYERS - 1, 1), :])
    write(NQ - 1).start()

    with jax.named_scope("outwait"):
        pltpu.make_async_copy(buf, dst, out_sem).wait()


def solution(mesh):
    y_count = mesh.shape[COL_AXIS]
    vol_spec = P(PARTS_AXIS, ROW_AXIS, COL_AXIS, None)
    any_spec = pl.BlockSpec(memory_space=pl.ANY)

    def local_layers(volume, filter_taps, mix_weights, mix_bias):
        vol = jnp.transpose(volume, (1, 2, 3, 0))
        toeplitz = (CH * ZL, WIN * ZL)
        passed_shapes = ((BX, BY, ZL, LANES), (QUAD, YS, ZL, LANES), toeplitz, (8 * BZ, 8 * BZ), (4 * C, 4 * C))
        passed = pl.pallas_call(
            functools.partial(kernel, y_count),
            out_shape=[jax.ShapeDtypeStruct(shape, BF16) for shape in passed_shapes],
            in_specs=[any_spec] * 4,
            out_specs=[any_spec] * 5,
            scratch_shapes=[
                pltpu.VMEM((BX, BY, BZ, C), BF16),
                pltpu.VMEM((LAYERS, XS, BY, ZL, LANES), BF16),
                pltpu.VMEM((LAYERS, BX, YS, ZL, LANES), BF16),
                pltpu.VMEM((CH * ZL, WIN * ZL), BF16),
                pltpu.VMEM((CH * ZL, WIN * ZL), BF16),
                pltpu.VMEM((8 * BZ, 8 * BZ), BF16),
                pltpu.VMEM((4 * C, 4 * C), BF16),
                pltpu.SMEM((LAYERS, 3, TAPS), F32),
                pltpu.VMEM((LAYERS, C, C), BF16),
                pltpu.VMEM((LAYERS, C), F32),
                pltpu.SemaphoreType.DMA((4,)),
                pltpu.SemaphoreType.DMA((3,)),
                pltpu.SemaphoreType.DMA,
                pltpu.SemaphoreType.DMA((2,)),
                pltpu.SemaphoreType.DMA((LAYERS, NQ)),
                pltpu.SemaphoreType.DMA((LAYERS,)),
                pltpu.SemaphoreType.DMA((LAYERS,)),
            ],
            compiler_params=pltpu.CompilerParams(collective_id=0, has_side_effects=True, vmem_limit_bytes=60 * 2**20),
        )(vol, filter_taps, mix_weights, mix_bias)
        result = pl.pallas_call(
            last_kernel,
            out_shape=jax.ShapeDtypeStruct((BX, BY, BZ, C), BF16),
            in_specs=[any_spec] * 6,
            out_specs=any_spec,
            scratch_shapes=[pltpu.VMEM(shape, BF16) for shape in passed_shapes] + [
                pltpu.VMEM((LAYERS, C), F32),
                pltpu.VMEM((BX, BY, BZ, C), BF16),
                pltpu.SemaphoreType.DMA((NQ,)),
                pltpu.SemaphoreType.DMA((5,)),
                pltpu.SemaphoreType.DMA,
            ],
            compiler_params=pltpu.CompilerParams(vmem_limit_bytes=60 * 2**20),
        )(*passed, mix_bias)
        return jnp.transpose(result, (3, 0, 1, 2))

    return jax.shard_map(local_layers, mesh=mesh, in_specs=(vol_spec, P(), P(), P()), out_specs=vol_spec, check_vma=False)
```

```python
import functools

import jax
import jax.numpy as jnp
from jax import lax
from jax.experimental import pallas as pl
from jax.experimental.pallas import tpu as pltpu
from jax.sharding import PartitionSpec as P

PARTS_AXIS = "batch"
COL_AXIS = "ysp"
ROW_AXIS = "xsp"
H = 10
TAPS = 2 * H + 1
LAYERS = 3
C = 64
BX = 32
BY = 32
BZ = 32
ZL = 16
LANES = 128
CH = 8
NCH = BX // CH
QUAD = 4
NQ = BX // QUAD
WIN = CH + 2 * H
EARLY = -(-(CH + H) // QUAD)
HEAD = QUAD + H
XS = BX + H
YS = BY + 2 * H
SEGS = ((BY - H, H), (0, H), (H, BY - 2 * H))
F32 = jnp.float32
BF16 = jnp.bfloat16


def band_times_eye(tap, rows, cols, inner, shift):
    i = lax.broadcasted_iota(jnp.int32, (rows, cols), 0)
    j = lax.broadcasted_iota(jnp.int32, (rows, cols), 1)
    t = j // inner - i // inner + shift
    acc = jnp.zeros((rows, cols), F32)
    for n in range(TAPS):
        acc = jnp.where(t == n, tap(n), acc)
    return jnp.where(i % inner == j % inner, acc, 0.0).astype(BF16)


def y_compute(window_of, old, put, ty, tz, w4, b):
    b = jnp.concatenate([b, b], axis=1)
    b = jnp.concatenate([b, b], axis=1)
    rs, ss = [], []
    for g in range(BY // 8):
        cols = [window_of(i, 8 * g).reshape(WIN * ZL, LANES) for i in range(QUAD)]
        rs.append(jnp.dot(ty[...], jnp.concatenate(cols, axis=1), preferred_element_type=F32).astype(BF16))
    for g in range(BY // 8):
        zs = []
        for i in range(QUAD):
            u = rs[g][:, LANES * i:LANES * (i + 1)].reshape(4, 2, ZL, LANES)
            ya, yb = u[:, 0], u[:, 1]
            lo = jnp.concatenate([ya[:, :, :C], yb[:, :, :C]], axis=2)
            hi = jnp.concatenate([ya[:, :, C:], yb[:, :, C:]], axis=2)
            zs.append(jnp.concatenate([lo, hi], axis=1).reshape(4 * BZ, LANES))
        dz = jnp.concatenate([jnp.concatenate(zs[:2], axis=0), jnp.concatenate(zs[2:], axis=0)], axis=1)
        ss.append(jnp.dot(tz[...], dz, preferred_element_type=F32).astype(BF16))
    for g in range(BY // 8):
        lhs = []
        for h in range(2):
            sh = ss[g][:, LANES * h:LANES * (h + 1)].reshape(8, 2, ZL, LANES)
            lhs.append(jnp.concatenate([sh[:, 0], sh[:, 1]], axis=2).reshape(8 * ZL, 2 * LANES))
        m = jnp.dot(jnp.concatenate(lhs, axis=0), w4[...], preferred_element_type=F32) + b
        m = jax.nn.gelu(m, approximate=True)
        for i in range(QUAD):
            mi = m[64 * i:64 * (i + 1)].reshape(4, 1, ZL, 2 * LANES)
            mi = jnp.concatenate([mi[..., :LANES], mi[..., LANES:]], axis=1).reshape(8, ZL, LANES)
            put(i, 8 * g, (old(i, 8 * g).astype(F32) + mi).astype(BF16))


def kernel(y_count, vol, taps_hbm, wmat_hbm, bias_hbm, out, u_out, ty_out, tz_out, w4_out, stage, vbuf, ubuf, tq, tx, ty, tz, w4, taps, wmat, bias, in_sem, small_sem, out_sem, ysend, yrecv, xsend, xrecv):
    xi = lax.axis_index(ROW_AXIS)
    yi = lax.axis_index(COL_AXIS)
    own = xi * H
    has_left = yi > 0
    has_right = yi < y_count - 1
    left = lax.rem(yi + y_count - 1, y_count)
    right = lax.rem(yi + 1, y_count)

    barrier = pltpu.get_barrier_semaphore()

    @pl.when(has_left)
    def _():
        pl.semaphore_signal(barrier, inc=1, device_id={COL_AXIS: left})

    @pl.when(has_right)
    def _():
        pl.semaphore_signal(barrier, inc=1, device_id={COL_AXIS: right})

    pl.semaphore_signal(barrier, inc=1, device_id={ROW_AXIS: 1 - xi})
    neighbours = 1 + has_left.astype(jnp.int32) + has_right.astype(jnp.int32)

    def x_of(k):
        return jnp.where(xi == 0, CH * k, BX - CH - CH * k)

    def xq_of(q):
        return jnp.where(xi == 0, QUAD * q, BX - QUAD - QUAD * q)

    x_head = jnp.where(xi == 0, 0, BX - HEAD)
    x_rest = jnp.where(xi == 0, HEAD, 0)

    def load(n):
        xs = pl.ds(x_rest, BX - HEAD) if n == 2 else pl.ds(x_head, HEAD)
        ys = pl.ds(0, BY) if n == 2 else pl.ds(*SEGS[min(n, 2)])
        return pltpu.make_async_copy(vol.at[xs, ys], stage.at[xs, ys], in_sem.at[n])

    small = [
        pltpu.make_async_copy(taps_hbm, taps, small_sem.at[0]),
        pltpu.make_async_copy(wmat_hbm, wmat, small_sem.at[1]),
        pltpu.make_async_copy(bias_hbm, bias, small_sem.at[2]),
    ]
    small[0].start()
    for n in range(4):
        load(n).start()
    small[1].start()
    small[2].start()

    def y_copy(l, q, side):
        xs = pl.ds(xq_of(q), QUAD)
        src = ubuf.at[l, xs, pl.ds(H, H)] if side == 0 else ubuf.at[l, xs, pl.ds(BY, H)]
        dst = ubuf.at[l, xs, pl.ds(H + BY, H)] if side == 0 else ubuf.at[l, xs, pl.ds(0, H)]
        return pltpu.make_async_remote_copy(
            src_ref=src, dst_ref=dst, send_sem=ysend.at[side], recv_sem=yrecv.at[l, q],
            device_id={COL_AXIS: left if side == 0 else right})

    def x_copy(l):
        src = jnp.where(xi == 0, BX - H, H)
        dst = jnp.where(xi == 0, 0, BX)
        return pltpu.make_async_remote_copy(
            src_ref=vbuf.at[l, pl.ds(src, H)], dst_ref=vbuf.at[l, pl.ds(dst, H)],
            send_sem=xsend.at[l], recv_sem=xrecv.at[l], device_id={ROW_AXIS: 1 - xi})

    def window(k):
        slot = own + x_of(k)
        return jnp.clip(slot - H, 0, XS - WIN), slot

    def x_mat(l, k):
        with jax.named_scope("xmat"):
            w0, slot = window(k)
            tx[...] = band_times_eye(lambda n: taps[l, 0, n], CH * ZL, WIN * ZL, ZL, w0 - slot + H)

    def x_rows(l, mat, w0, width, x0, count, seg):
        with jax.named_scope("xseg"):
            first, ny = SEGS[seg]
            cols = [vbuf[l, pl.ds(w0, width), first + i].reshape(width * ZL, LANES) for i in range(ny)]
            r = jnp.dot(mat, jnp.concatenate(cols, axis=1), preferred_element_type=F32).astype(BF16)
            for i in range(ny):
                ubuf[l, pl.ds(x0, count), H + first + i] = r[:, LANES * i:LANES * (i + 1)].reshape(count, ZL, LANES)

    def x_seg(l, k, seg):
        w0, _ = window(k)
        x_rows(l, tx[...], w0, WIN, x_of(k), CH, seg)

    def last_copy(side):
        l, q = LAYERS - 1, NQ - 1
        src = ubuf.at[l, pl.ds(xq_of(q), QUAD), pl.ds(H if side == 0 else BY, H)]
        return pltpu.make_async_remote_copy(
            src_ref=src, dst_ref=u_out.at[:, pl.ds(H + BY if side == 0 else 0, H)], send_sem=ysend.at[side], recv_sem=yrecv.at[l, q],
            device_id={COL_AXIS: left if side == 0 else right})

    def send_quad(l, q, side):
        goes = has_left if side == 0 else has_right
        last = (l == LAYERS - 1) & (q == NQ - 1)

        @pl.when(goes & jnp.logical_not(last))
        def _():
            y_copy(l, q, side).start()

        @pl.when(goes & last)
        def _():
            last_copy(side).start()

    def y_send(l, k, side):
        for j in range(CH // QUAD):
            send_quad(l, k * (CH // QUAD) + j, side)

    def x_pass(l, k):
        x_mat(l, k)
        x_seg(l, k, 0)
        y_send(l, k, 1)
        x_seg(l, k, 1)
        y_send(l, k, 0)
        x_seg(l, k, 2)

    def layer_mats(l):
        ty[...] = band_times_eye(lambda n: taps[l, 1, n], CH * ZL, WIN * ZL, ZL, 0)
        i = lax.broadcasted_iota(jnp.int32, (8 * BZ, 8 * BZ), 0)
        j = lax.broadcasted_iota(jnp.int32, (8 * BZ, 8 * BZ), 1)
        t = j - i + H
        acc = jnp.zeros((8 * BZ, 8 * BZ), F32)
        for n in range(TAPS):
            acc = jnp.where(t == n, taps[l, 2, n], acc)
        tz[...] = jnp.where(i // BZ == j // BZ, acc, 0.0).astype(BF16)
        w = wmat[l].astype(F32)
        w = jnp.concatenate([w, w], axis=1)
        w = jnp.concatenate([w, w], axis=1)
        w = jnp.concatenate([w, w, w, w], axis=0)
        i = lax.broadcasted_iota(jnp.int32, (4 * C, 4 * C), 0) // C
        j = lax.broadcasted_iota(jnp.int32, (4 * C, 4 * C), 1) // C
        keep = (i // 2 == j % 2) & (i % 2 == j // 2)
        w4[...] = jnp.where(keep, w, 0.0).astype(BF16)

    def y_wait(l, q):
        with jax.named_scope("ywait"):
            both = ubuf.at[l, pl.ds(xq_of(q), QUAD), pl.ds(0, 2 * H)]

            @pl.when(has_left & has_right)
            def _():
                pltpu.make_async_remote_copy(
                    src_ref=both, dst_ref=both, send_sem=ysend.at[0], recv_sem=yrecv.at[l, q],
                    device_id={COL_AXIS: left}).wait_recv()

            @pl.when(jnp.logical_not(has_left & has_right))
            def _():
                y_copy(l, q, 0).wait_recv()

    def y_quad(l, q):
        y_wait(l, q)
        with jax.named_scope("yquad"):
            xq = xq_of(q)
            nxt = jnp.minimum(l + 1, LAYERS - 1)

            def window_of(i, y0):
                return ubuf[l, xq + i, pl.ds(y0, WIN)]

            def old(i, y0):
                return vbuf[l, own + xq + i, pl.ds(y0, 8)]

            def put(i, y0, v):
                vbuf[nxt, own + xq + i, pl.ds(y0, 8)] = v

            y_compute(window_of, old, put, ty, tz, w4, bias[pl.ds(l, 1), :])

    def zero_planes(l):
        vbuf[l, pl.ds(own + jnp.where(xi == 0, QUAD * EARLY, 0), BX - QUAD * EARLY)] = jnp.zeros((BX - QUAD * EARLY, BY, ZL, LANES), BF16)

    def zero_halo(l, y0):
        def body(n, carry):
            ubuf[l, n, pl.ds(y0, H)] = jnp.zeros((H, ZL, LANES), BF16)
            return carry

        lax.fori_loop(0, BX, body, 0)

    def pack(n, x0, count, first, ny):
        with jax.named_scope("pack"):
            ys = pl.ds(first, ny)

            def body(p, c):
                s = stage[x0 + p, ys]
                vbuf[0, own + x0 + p, ys] = jnp.concatenate([s[:, :ZL], s[:, ZL:]], axis=2)
                return c

            lax.fori_loop(0, count, body, 0, unroll=True)

    small[0].wait()
    slot = own + xq_of(0)
    w0 = own + x_head
    tq[...] = band_times_eye(lambda n: taps[0, 0, n], QUAD * ZL, HEAD * ZL, ZL, w0 - slot + H)
    for seg in range(2):
        load(seg).wait()
        pack(seg, x_head, HEAD, *SEGS[seg])
        x_rows(0, tq[...], w0, HEAD, xq_of(0), QUAD, seg)
        if seg == 0:
            with jax.named_scope("barrier"):
                pl.semaphore_wait(barrier, neighbours)
        send_quad(0, 0, 1 - seg)
    x_mat(0, 0)
    load(2).wait()
    pack(2, x_rest, BX - HEAD, 0, BY)
    x_copy(0).start()
    second = tx[pl.ds(jnp.where(xi == 0, QUAD * ZL, 0), QUAD * ZL), :]
    for seg in range(2):
        x_rows(0, second, window(0)[0], WIN, xq_of(1), QUAD, seg)
        send_quad(0, 1, 1 - seg)
    load(3).wait()
    pack(3, x_head, HEAD, *SEGS[2])
    x_seg(0, 0, 2)
    x_pass(0, 1)
    for l in range(1, LAYERS):
        zero_planes(l)
    small[1].wait()
    small[2].wait()

    def layer(l, carry):
        def xs(k, c):
            @pl.when(k == 2)
            def _():
                with jax.named_scope("xwait"):
                    x_copy(l).wait()

            x_pass(l, k)
            return c

        lax.fori_loop(2, NCH, xs, 0)
        with jax.named_scope("mats"):
            layer_mats(l)

        @pl.when(jnp.logical_not(has_left))
        def _():
            zero_halo(l, 0)

        @pl.when(jnp.logical_not(has_right))
        def _():
            zero_halo(l, H + BY)

        @pl.when(l == LAYERS - 1)
        def _():
            store(NQ - 1).start()
            for mat in store_mats:
                mat.start()
            store_u.start()
            for edge, copy in store_edges:
                pl.when(edge)(copy.start)

        def ys(q, c):
            @pl.when(((q == EARLY) | (q == NQ - 1)) & (l < LAYERS - 1))
            def _():
                x_pass(l + 1, jnp.where(q == EARLY, 0, 1))

            @pl.when((q < NQ - 1) | (l < LAYERS - 1))
            def _():
                y_quad(l, q)

            @pl.when((q < NQ - 1) & (l == LAYERS - 1))
            def _():
                store(q).start()

            return c

        lax.fori_loop(0, NQ, ys, 0)

        @pl.when(l < LAYERS - 1)
        def _():
            x_copy(l + 1).start()

        return carry

    def store(q):
        xs = xq_of(q)
        return pltpu.make_async_copy(vbuf.at[LAYERS - 1, pl.ds(own + xs, QUAD)], out.at[pl.ds(xs, QUAD)], out_sem)

    store_mats = [pltpu.make_async_copy(m, o, small_sem.at[n]) for n, (m, o) in enumerate(((ty, ty_out), (tz, tz_out), (w4, w4_out)))]
    last_u = ubuf.at[LAYERS - 1, pl.ds(xq_of(NQ - 1), QUAD)]
    store_u = pltpu.make_async_copy(last_u.at[:, pl.ds(H, BY)], u_out.at[:, pl.ds(H, BY)], in_sem.at[0])
    store_edges = [
        (jnp.logical_not(has), pltpu.make_async_copy(last_u.at[:, pl.ds(y0, H)], u_out.at[:, pl.ds(y0, H)], in_sem.at[n]))
        for has, y0, n in ((has_left, 0, 2), (has_right, H + BY, 3))
    ]
    lax.fori_loop(0, LAYERS, layer, 0)
    y_wait(LAYERS - 1, NQ - 1)

    with jax.named_scope("finish"):
        for side in range(2):
            sent = ubuf.at[:, :, pl.ds(0, H)]

            @pl.when(has_left if side == 0 else has_right)
            def _():
                pltpu.make_async_remote_copy(
                    src_ref=sent, dst_ref=sent, send_sem=ysend.at[side], recv_sem=yrecv.at[0, 0],
                    device_id={COL_AXIS: left if side == 0 else right}).wait_send()

        pltpu.make_async_copy(vbuf.at[LAYERS - 1, pl.ds(own, BX)], out, out_sem).wait()
        for edge, copy in store_edges:
            pl.when(edge)(copy.wait)
        for mat in store_mats:
            mat.wait()
        store_u.wait()


def unpack(s):
    r = pltpu.roll(s.reshape(QUAD * BY * ZL, LANES), C, 1).reshape(QUAD, BY, ZL, LANES)
    return s[:, :, :, :C], r[:, :, :, :C]


def last_kernel(src, u_hbm, ty_hbm, tz_hbm, w4_hbm, bias_hbm, dst, got, u, ty, tz, w4, bias, buf, in_sems, mat_sems, out_sem):
    xi = lax.axis_index(ROW_AXIS)

    def planes(q):
        return pl.ds(jnp.where(xi == 0, QUAD * q, BX - QUAD - QUAD * q), QUAD)

    def read(q):
        return pltpu.make_async_copy(src.at[planes(q)], got.at[planes(q)], in_sems.at[q])

    def write(q):
        return pltpu.make_async_copy(buf.at[planes(q)], dst.at[planes(q)], out_sem)

    mats = [
        pltpu.make_async_copy(h, v, mat_sems.at[n])
        for n, (h, v) in enumerate(((u_hbm, u), (ty_hbm, ty), (tz_hbm, tz), (w4_hbm, w4), (bias_hbm, bias)))
    ]
    for q in range(NQ - 1):
        read(q).start()
    for mat in mats:
        mat.start()
    read(NQ - 1).start()

    def body(q, carry):
        read(q).wait()
        buf[planes(q), :, :ZL, :], buf[planes(q), :, ZL:, :] = unpack(got[planes(q)])
        write(q).start()
        return carry

    with jax.named_scope("unpack"):
        lax.fori_loop(0, NQ - 1, body, 0)
    with jax.named_scope("matwait"):
        for mat in mats:
            mat.wait()
        read(NQ - 1).wait()
    xq = jnp.where(xi == 0, BX - QUAD, 0)

    def put(i, y0, v):
        buf[xq + i, pl.ds(y0, 8), :ZL, :] = v[:, :, :C]
        buf[xq + i, pl.ds(y0, 8), ZL:, :] = v[:, :, C:]

    with jax.named_scope("ycomp"):
        y_compute(
            lambda i, y0: u[i, pl.ds(y0, WIN)], lambda i, y0: got[xq + i, pl.ds(y0, 8)], put,
            ty, tz, w4, bias[pl.ds(LAYERS - 1, 1), :])
    write(NQ - 1).start()

    with jax.named_scope("outwait"):
        pltpu.make_async_copy(buf, dst, out_sem).wait()


def solution(mesh):
    y_count = mesh.shape[COL_AXIS]
    vol_spec = P(PARTS_AXIS, ROW_AXIS, COL_AXIS, None)
    any_spec = pl.BlockSpec(memory_space=pl.ANY)

    def local_layers(volume, filter_taps, mix_weights, mix_bias):
        vol = jnp.transpose(volume, (1, 2, 3, 0))
        toeplitz = (CH * ZL, WIN * ZL)
        passed_shapes = ((BX, BY, ZL, LANES), (QUAD, YS, ZL, LANES), toeplitz, (8 * BZ, 8 * BZ), (4 * C, 4 * C))
        passed = pl.pallas_call(
            functools.partial(kernel, y_count),
            out_shape=[jax.ShapeDtypeStruct(shape, BF16) for shape in passed_shapes],
            in_specs=[any_spec] * 4,
            out_specs=[any_spec] * 5,
            scratch_shapes=[
                pltpu.VMEM((BX, BY, BZ, C), BF16),
                pltpu.VMEM((LAYERS, XS, BY, ZL, LANES), BF16),
                pltpu.VMEM((LAYERS, BX, YS, ZL, LANES), BF16),
                pltpu.VMEM((QUAD * ZL, HEAD * ZL), BF16),
                pltpu.VMEM(toeplitz, BF16),
                pltpu.VMEM(toeplitz, BF16),
                pltpu.VMEM((8 * BZ, 8 * BZ), BF16),
                pltpu.VMEM((4 * C, 4 * C), BF16),
                pltpu.SMEM((LAYERS, 3, TAPS), F32),
                pltpu.VMEM((LAYERS, C, C), BF16),
                pltpu.VMEM((LAYERS, C), F32),
                pltpu.SemaphoreType.DMA((4,)),
                pltpu.SemaphoreType.DMA((3,)),
                pltpu.SemaphoreType.DMA,
                pltpu.SemaphoreType.DMA((2,)),
                pltpu.SemaphoreType.DMA((LAYERS, NQ)),
                pltpu.SemaphoreType.DMA((LAYERS,)),
                pltpu.SemaphoreType.DMA((LAYERS,)),
            ],
            compiler_params=pltpu.CompilerParams(collective_id=0, has_side_effects=True, vmem_limit_bytes=60 * 2**20),
        )(vol, filter_taps, mix_weights, mix_bias)
        result = pl.pallas_call(
            last_kernel,
            out_shape=jax.ShapeDtypeStruct((BX, BY, BZ, C), BF16),
            in_specs=[any_spec] * 6,
            out_specs=any_spec,
            scratch_shapes=[pltpu.VMEM(shape, BF16) for shape in passed_shapes] + [
                pltpu.VMEM((LAYERS, C), F32),
                pltpu.VMEM((BX, BY, BZ, C), BF16),
                pltpu.SemaphoreType.DMA((NQ,)),
                pltpu.SemaphoreType.DMA((5,)),
                pltpu.SemaphoreType.DMA,
            ],
            compiler_params=pltpu.CompilerParams(vmem_limit_bytes=60 * 2**20),
        )(*passed, mix_bias)
        return jnp.transpose(result, (3, 0, 1, 2))

    return jax.shard_map(local_layers, mesh=mesh, in_specs=(vol_spec, P(), P(), P()), out_specs=vol_spec, check_vma=False)
```

```python
import functools

import jax
import jax.numpy as jnp
from jax import lax
from jax.experimental import pallas as pl
from jax.experimental.pallas import tpu as pltpu
from jax.sharding import PartitionSpec as P

PARTS_AXIS = "batch"
COL_AXIS = "ysp"
ROW_AXIS = "xsp"
H = 10
TAPS = 2 * H + 1
LAYERS = 3
C = 64
BX = 32
BY = 32
BZ = 32
ZL = 16
LANES = 128
CH = 8
NCH = BX // CH
QUAD = 4
NQ = BX // QUAD
WIN = CH + 2 * H
BEFORE = 5
EARLY = -(-(CH + H) // QUAD)
HEAD = QUAD + H
XS = BX + H
YS = BY + 2 * H
SEGS = ((BY - H, H), (0, H), (H, BY - 2 * H))
F32 = jnp.float32
BF16 = jnp.bfloat16


def band_times_eye(tap, rows, cols, inner, shift):
    i = lax.broadcasted_iota(jnp.int32, (rows, cols), 0)
    j = lax.broadcasted_iota(jnp.int32, (rows, cols), 1)
    t = j // inner - i // inner + shift
    acc = jnp.zeros((rows, cols), F32)
    for n in range(TAPS):
        acc = jnp.where(t == n, tap(n), acc)
    return jnp.where(i % inner == j % inner, acc, 0.0).astype(BF16)


def y_compute(window_of, old, put, ty, tz, w4, b, between=lambda stage: None):
    b = jnp.concatenate([b, b], axis=1)
    b = jnp.concatenate([b, b], axis=1)
    rs, ss = [], []
    for g in range(BY // 8):
        cols = [window_of(i, 8 * g).reshape(WIN * ZL, LANES) for i in range(QUAD)]
        rs.append(jnp.dot(ty[...], jnp.concatenate(cols, axis=1), preferred_element_type=F32).astype(BF16))
    between(0)
    for g in range(BY // 8):
        zs = []
        for i in range(QUAD):
            u = rs[g][:, LANES * i:LANES * (i + 1)].reshape(4, 2, ZL, LANES)
            ya, yb = u[:, 0], u[:, 1]
            lo = jnp.concatenate([ya[:, :, :C], yb[:, :, :C]], axis=2)
            hi = jnp.concatenate([ya[:, :, C:], yb[:, :, C:]], axis=2)
            zs.append(jnp.concatenate([lo, hi], axis=1).reshape(4 * BZ, LANES))
        dz = jnp.concatenate([jnp.concatenate(zs[:2], axis=0), jnp.concatenate(zs[2:], axis=0)], axis=1)
        ss.append(jnp.dot(tz[...], dz, preferred_element_type=F32).astype(BF16))
    between(1)
    for g in range(BY // 8):
        lhs = []
        for h in range(2):
            sh = ss[g][:, LANES * h:LANES * (h + 1)].reshape(8, 2, ZL, LANES)
            lhs.append(jnp.concatenate([sh[:, 0], sh[:, 1]], axis=2).reshape(8 * ZL, 2 * LANES))
        m = jnp.dot(jnp.concatenate(lhs, axis=0), w4[...], preferred_element_type=F32) + b
        m = jax.nn.gelu(m, approximate=True)
        for i in range(QUAD):
            mi = m[64 * i:64 * (i + 1)].reshape(4, 1, ZL, 2 * LANES)
            mi = jnp.concatenate([mi[..., :LANES], mi[..., LANES:]], axis=1).reshape(8, ZL, LANES)
            put(i, 8 * g, (old(i, 8 * g).astype(F32) + mi).astype(BF16))


def kernel(y_count, vol, taps_hbm, wmat_hbm, bias_hbm, out, u_out, ty_out, tz_out, w4_out, stage, vbuf, ubuf, tq, tx, ty, tz, w4, taps, wmat, bias, in_sem, small_sem, out_sem, ysend, yrecv, xsend, xrecv):
    xi = lax.axis_index(ROW_AXIS)
    yi = lax.axis_index(COL_AXIS)
    own = xi * H
    has_left = yi > 0
    has_right = yi < y_count - 1
    left = lax.rem(yi + y_count - 1, y_count)
    right = lax.rem(yi + 1, y_count)

    barrier = pltpu.get_barrier_semaphore()

    @pl.when(has_left)
    def _():
        pl.semaphore_signal(barrier, inc=1, device_id={COL_AXIS: left})

    @pl.when(has_right)
    def _():
        pl.semaphore_signal(barrier, inc=1, device_id={COL_AXIS: right})

    pl.semaphore_signal(barrier, inc=1, device_id={ROW_AXIS: 1 - xi})
    neighbours = 1 + has_left.astype(jnp.int32) + has_right.astype(jnp.int32)

    def x_of(k):
        return jnp.where(xi == 0, CH * k, BX - CH - CH * k)

    def xq_of(q):
        return jnp.where(xi == 0, QUAD * q, BX - QUAD - QUAD * q)

    x_head = jnp.where(xi == 0, 0, BX - HEAD)
    x_rest = jnp.where(xi == 0, HEAD, 0)

    def load(n):
        xs = pl.ds(x_rest, BX - HEAD) if n == 2 else pl.ds(x_head, HEAD)
        ys = pl.ds(0, BY) if n == 2 else pl.ds(*SEGS[min(n, 2)])
        return pltpu.make_async_copy(vol.at[xs, ys], stage.at[xs, ys], in_sem.at[n])

    small = [
        pltpu.make_async_copy(taps_hbm, taps, small_sem.at[0]),
        pltpu.make_async_copy(wmat_hbm, wmat, small_sem.at[1]),
        pltpu.make_async_copy(bias_hbm, bias, small_sem.at[2]),
    ]
    small[0].start()
    for n in range(4):
        load(n).start()
    small[1].start()
    small[2].start()

    def y_copy(l, q, side):
        xs = pl.ds(xq_of(q), QUAD)
        src = ubuf.at[l, xs, pl.ds(H, H)] if side == 0 else ubuf.at[l, xs, pl.ds(BY, H)]
        dst = ubuf.at[l, xs, pl.ds(H + BY, H)] if side == 0 else ubuf.at[l, xs, pl.ds(0, H)]
        return pltpu.make_async_remote_copy(
            src_ref=src, dst_ref=dst, send_sem=ysend.at[side], recv_sem=yrecv.at[l, q],
            device_id={COL_AXIS: left if side == 0 else right})

    def x_copy(l):
        src = jnp.where(xi == 0, BX - H, H)
        dst = jnp.where(xi == 0, 0, BX)
        return pltpu.make_async_remote_copy(
            src_ref=vbuf.at[l, pl.ds(src, H)], dst_ref=vbuf.at[l, pl.ds(dst, H)],
            send_sem=xsend.at[l], recv_sem=xrecv.at[l], device_id={ROW_AXIS: 1 - xi})

    def window(k):
        slot = own + x_of(k)
        return jnp.clip(slot - H, 0, XS - WIN), slot

    def x_mat(l, k):
        with jax.named_scope("xmat"):
            w0, slot = window(k)
            tx[...] = band_times_eye(lambda n: taps[l, 0, n], CH * ZL, WIN * ZL, ZL, w0 - slot + H)

    def x_rows(l, mat, w0, width, x0, count, seg):
        with jax.named_scope("xseg"):
            first, ny = SEGS[seg]
            cols = [vbuf[l, pl.ds(w0, width), first + i].reshape(width * ZL, LANES) for i in range(ny)]
            r = jnp.dot(mat, jnp.concatenate(cols, axis=1), preferred_element_type=F32).astype(BF16)
            for i in range(ny):
                ubuf[l, pl.ds(x0, count), H + first + i] = r[:, LANES * i:LANES * (i + 1)].reshape(count, ZL, LANES)

    def x_seg(l, k, seg):
        w0, _ = window(k)
        x_rows(l, tx[...], w0, WIN, x_of(k), CH, seg)

    def last_copy(side):
        l, q = LAYERS - 1, NQ - 1
        src = ubuf.at[l, pl.ds(xq_of(q), QUAD), pl.ds(H if side == 0 else BY, H)]
        return pltpu.make_async_remote_copy(
            src_ref=src, dst_ref=u_out.at[:, pl.ds(H + BY if side == 0 else 0, H)], send_sem=ysend.at[side], recv_sem=yrecv.at[l, q],
            device_id={COL_AXIS: left if side == 0 else right})

    def send_quad(l, q, side):
        goes = has_left if side == 0 else has_right
        last = (l == LAYERS - 1) & (q == NQ - 1)

        @pl.when(goes & jnp.logical_not(last))
        def _():
            y_copy(l, q, side).start()

        @pl.when(goes & last)
        def _():
            last_copy(side).start()

    def y_send(l, k, side):
        for j in range(CH // QUAD):
            send_quad(l, k * (CH // QUAD) + j, side)

    def x_pass(l, k):
        x_mat(l, k)
        x_seg(l, k, 0)
        y_send(l, k, 1)
        x_seg(l, k, 1)
        y_send(l, k, 0)
        x_seg(l, k, 2)

    def layer_mats(l):
        ty[...] = band_times_eye(lambda n: taps[l, 1, n], CH * ZL, WIN * ZL, ZL, 0)
        i = lax.broadcasted_iota(jnp.int32, (8 * BZ, 8 * BZ), 0)
        j = lax.broadcasted_iota(jnp.int32, (8 * BZ, 8 * BZ), 1)
        t = j - i + H
        acc = jnp.zeros((8 * BZ, 8 * BZ), F32)
        for n in range(TAPS):
            acc = jnp.where(t == n, taps[l, 2, n], acc)
        tz[...] = jnp.where(i // BZ == j // BZ, acc, 0.0).astype(BF16)
        w = wmat[l].astype(F32)
        w = jnp.concatenate([w, w], axis=1)
        w = jnp.concatenate([w, w], axis=1)
        w = jnp.concatenate([w, w, w, w], axis=0)
        i = lax.broadcasted_iota(jnp.int32, (4 * C, 4 * C), 0) // C
        j = lax.broadcasted_iota(jnp.int32, (4 * C, 4 * C), 1) // C
        keep = (i // 2 == j % 2) & (i % 2 == j // 2)
        w4[...] = jnp.where(keep, w, 0.0).astype(BF16)

    def y_wait(l, q):
        with jax.named_scope("ywait"):
            both = ubuf.at[l, pl.ds(xq_of(q), QUAD), pl.ds(0, 2 * H)]

            @pl.when(has_left & has_right)
            def _():
                pltpu.make_async_remote_copy(
                    src_ref=both, dst_ref=both, send_sem=ysend.at[0], recv_sem=yrecv.at[l, q],
                    device_id={COL_AXIS: left}).wait_recv()

            @pl.when(jnp.logical_not(has_left & has_right))
            def _():
                y_copy(l, q, 0).wait_recv()

    def y_quad(l, q):
        y_wait(l, q)
        with jax.named_scope("yquad"):
            xq = xq_of(q)
            nxt = jnp.minimum(l + 1, LAYERS - 1)

            def window_of(i, y0):
                return ubuf[l, xq + i, pl.ds(y0, WIN)]

            def old(i, y0):
                return vbuf[l, own + xq + i, pl.ds(y0, 8)]

            def put(i, y0, v):
                vbuf[nxt, own + xq + i, pl.ds(y0, 8)] = v

            y_compute(window_of, old, put, ty, tz, w4, bias[pl.ds(l, 1), :])

    def zero_planes(l):
        vbuf[l, pl.ds(own + jnp.where(xi == 0, QUAD * EARLY, 0), BX - QUAD * EARLY)] = jnp.zeros((BX - QUAD * EARLY, BY, ZL, LANES), BF16)

    def zero_halo(l, y0):
        def body(n, carry):
            ubuf[l, n, pl.ds(y0, H)] = jnp.zeros((H, ZL, LANES), BF16)
            return carry

        lax.fori_loop(0, BX, body, 0)

    def pack(n, x0, count, first, ny):
        with jax.named_scope("pack"):
            ys = pl.ds(first, ny)

            def body(p, c):
                s = stage[x0 + p, ys]
                vbuf[0, own + x0 + p, ys] = jnp.concatenate([s[:, :ZL], s[:, ZL:]], axis=2)
                return c

            lax.fori_loop(0, count, body, 0, unroll=True)

    small[0].wait()
    slot = own + xq_of(0)
    w0 = own + x_head
    tq[...] = band_times_eye(lambda n: taps[0, 0, n], QUAD * ZL, HEAD * ZL, ZL, w0 - slot + H)
    for seg in range(2):
        load(seg).wait()
        pack(seg, x_head, HEAD, *SEGS[seg])
        x_rows(0, tq[...], w0, HEAD, xq_of(0), QUAD, seg)
        if seg == 0:
            with jax.named_scope("barrier"):
                pl.semaphore_wait(barrier, neighbours)
        send_quad(0, 0, 1 - seg)
    x_mat(0, 0)
    load(2).wait()
    pack(2, x_rest, BX - HEAD, 0, BY)
    x_copy(0).start()
    second = tx[pl.ds(jnp.where(xi == 0, QUAD * ZL, 0), QUAD * ZL), :]
    for seg in range(2):
        x_rows(0, second, window(0)[0], WIN, xq_of(1), QUAD, seg)
        send_quad(0, 1, 1 - seg)
    load(3).wait()
    pack(3, x_head, HEAD, *SEGS[2])
    x_seg(0, 0, 2)
    x_pass(0, 1)
    for l in range(1, LAYERS):
        zero_planes(l)
    small[1].wait()
    small[2].wait()

    def layer(l, carry):
        def xs(k, c):
            @pl.when(k == 2)
            def _():
                with jax.named_scope("xwait"):
                    x_copy(l).wait()

            x_pass(l, k)
            return c

        lax.fori_loop(2, NCH, xs, 0)
        with jax.named_scope("mats"):
            layer_mats(l)

        @pl.when(jnp.logical_not(has_left))
        def _():
            zero_halo(l, 0)

        @pl.when(jnp.logical_not(has_right))
        def _():
            zero_halo(l, H + BY)

        @pl.when(l == LAYERS - 1)
        def _():
            store(NQ - 1).start()
            for mat in store_mats:
                mat.start()
            store_u.start()
            for edge, copy in store_edges:
                pl.when(edge)(copy.start)

        def ys(q, c):
            @pl.when(((q == EARLY) | (q == NQ - 1)) & (l < LAYERS - 1))
            def _():
                x_pass(l + 1, jnp.where(q == EARLY, 0, 1))

            @pl.when((q < NQ - 1) | (l < LAYERS - 1))
            def _():
                y_quad(l, q)

            @pl.when((q < NQ - 1) & (l == LAYERS - 1))
            def _():
                store(q).start()

            return c

        lax.fori_loop(0, NQ, ys, 0)

        @pl.when(l < LAYERS - 1)
        def _():
            x_copy(l + 1).start()

        return carry

    def store(q):
        xs = xq_of(q)
        return pltpu.make_async_copy(vbuf.at[LAYERS - 1, pl.ds(own + xs, QUAD)], out.at[pl.ds(xs, QUAD)], out_sem)

    store_mats = [pltpu.make_async_copy(m, o, small_sem.at[n]) for n, (m, o) in enumerate(((ty, ty_out), (tz, tz_out), (w4, w4_out)))]
    last_u = ubuf.at[LAYERS - 1, pl.ds(xq_of(NQ - 1), QUAD)]
    store_u = pltpu.make_async_copy(last_u.at[:, pl.ds(H, BY)], u_out.at[:, pl.ds(H, BY)], in_sem.at[0])
    store_edges = [
        (jnp.logical_not(has), pltpu.make_async_copy(last_u.at[:, pl.ds(y0, H)], u_out.at[:, pl.ds(y0, H)], in_sem.at[n]))
        for has, y0, n in ((has_left, 0, 2), (has_right, H + BY, 3))
    ]
    lax.fori_loop(0, LAYERS, layer, 0)
    y_wait(LAYERS - 1, NQ - 1)

    with jax.named_scope("finish"):
        for side in range(2):
            sent = ubuf.at[:, :, pl.ds(0, H)]

            @pl.when(has_left if side == 0 else has_right)
            def _():
                pltpu.make_async_remote_copy(
                    src_ref=sent, dst_ref=sent, send_sem=ysend.at[side], recv_sem=yrecv.at[0, 0],
                    device_id={COL_AXIS: left if side == 0 else right}).wait_send()

        pltpu.make_async_copy(vbuf.at[LAYERS - 1, pl.ds(own, BX)], out, out_sem).wait()
        for edge, copy in store_edges:
            pl.when(edge)(copy.wait)
        for mat in store_mats:
            mat.wait()
        store_u.wait()


def unpack(s):
    r = pltpu.roll(s.reshape(QUAD * BY * ZL, LANES), C, 1).reshape(QUAD, BY, ZL, LANES)
    return s[:, :, :, :C], r[:, :, :, :C]


def last_kernel(src, u_hbm, ty_hbm, tz_hbm, w4_hbm, bias_hbm, dst, got, u, ty, tz, w4, bias, buf, in_sems, mat_sems, out_sem):
    xi = lax.axis_index(ROW_AXIS)

    def planes(q):
        return pl.ds(jnp.where(xi == 0, QUAD * q, BX - QUAD - QUAD * q), QUAD)

    def read(q):
        return pltpu.make_async_copy(src.at[planes(q)], got.at[planes(q)], in_sems.at[q])

    def write(q):
        return pltpu.make_async_copy(buf.at[planes(q)], dst.at[planes(q)], out_sem)

    mats = [
        pltpu.make_async_copy(h, v, mat_sems.at[n])
        for n, (h, v) in enumerate(((u_hbm, u), (ty_hbm, ty), (tz_hbm, tz), (w4_hbm, w4), (bias_hbm, bias)))
    ]
    for q in range(NQ - 1):
        read(q).start()
    for mat in mats:
        mat.start()
    read(NQ - 1).start()

    def turn(q):
        buf[planes(q), :, :ZL, :], buf[planes(q), :, ZL:, :] = unpack(got[planes(q)])

    def body(q, carry):
        read(q).wait()
        turn(q)
        write(q).start()
        return carry

    def between(stage):
        for q in range(BEFORE, NQ - 1):
            if stage == 0:
                turn(q)
            else:
                write(q).start()

    with jax.named_scope("unpack"):
        lax.fori_loop(0, BEFORE, body, 0)
        for q in range(BEFORE, NQ - 1):
            read(q).wait()
    with jax.named_scope("matwait"):
        for mat in mats:
            mat.wait()
        read(NQ - 1).wait()
    xq = jnp.where(xi == 0, BX - QUAD, 0)

    def put(i, y0, v):
        buf[xq + i, pl.ds(y0, 8), :ZL, :] = v[:, :, :C]
        buf[xq + i, pl.ds(y0, 8), ZL:, :] = v[:, :, C:]

    with jax.named_scope("ycomp"):
        y_compute(
            lambda i, y0: u[i, pl.ds(y0, WIN)], lambda i, y0: got[xq + i, pl.ds(y0, 8)], put,
            ty, tz, w4, bias[pl.ds(LAYERS - 1, 1), :], between)
    write(NQ - 1).start()

    with jax.named_scope("outwait"):
        pltpu.make_async_copy(buf, dst, out_sem).wait()


def solution(mesh):
    y_count = mesh.shape[COL_AXIS]
    vol_spec = P(PARTS_AXIS, ROW_AXIS, COL_AXIS, None)
    any_spec = pl.BlockSpec(memory_space=pl.ANY)

    def local_layers(volume, filter_taps, mix_weights, mix_bias):
        vol = jnp.transpose(volume, (1, 2, 3, 0))
        toeplitz = (CH * ZL, WIN * ZL)
        passed_shapes = ((BX, BY, ZL, LANES), (QUAD, YS, ZL, LANES), toeplitz, (8 * BZ, 8 * BZ), (4 * C, 4 * C))
        passed = pl.pallas_call(
            functools.partial(kernel, y_count),
            out_shape=[jax.ShapeDtypeStruct(shape, BF16) for shape in passed_shapes],
            in_specs=[any_spec] * 4,
            out_specs=[any_spec] * 5,
            scratch_shapes=[
                pltpu.VMEM((BX, BY, BZ, C), BF16),
                pltpu.VMEM((LAYERS, XS, BY, ZL, LANES), BF16),
                pltpu.VMEM((LAYERS, BX, YS, ZL, LANES), BF16),
                pltpu.VMEM((QUAD * ZL, HEAD * ZL), BF16),
                pltpu.VMEM(toeplitz, BF16),
                pltpu.VMEM(toeplitz, BF16),
                pltpu.VMEM((8 * BZ, 8 * BZ), BF16),
                pltpu.VMEM((4 * C, 4 * C), BF16),
                pltpu.SMEM((LAYERS, 3, TAPS), F32),
                pltpu.VMEM((LAYERS, C, C), BF16),
                pltpu.VMEM((LAYERS, C), F32),
                pltpu.SemaphoreType.DMA((4,)),
                pltpu.SemaphoreType.DMA((3,)),
                pltpu.SemaphoreType.DMA,
                pltpu.SemaphoreType.DMA((2,)),
                pltpu.SemaphoreType.DMA((LAYERS, NQ)),
                pltpu.SemaphoreType.DMA((LAYERS,)),
                pltpu.SemaphoreType.DMA((LAYERS,)),
            ],
            compiler_params=pltpu.CompilerParams(collective_id=0, has_side_effects=True, vmem_limit_bytes=60 * 2**20),
        )(vol, filter_taps, mix_weights, mix_bias)
        result = pl.pallas_call(
            last_kernel,
            out_shape=jax.ShapeDtypeStruct((BX, BY, BZ, C), BF16),
            in_specs=[any_spec] * 6,
            out_specs=any_spec,
            scratch_shapes=[pltpu.VMEM(shape, BF16) for shape in passed_shapes] + [
                pltpu.VMEM((LAYERS, C), F32),
                pltpu.VMEM((BX, BY, BZ, C), BF16),
                pltpu.SemaphoreType.DMA((NQ,)),
                pltpu.SemaphoreType.DMA((5,)),
                pltpu.SemaphoreType.DMA,
            ],
            compiler_params=pltpu.CompilerParams(vmem_limit_bytes=60 * 2**20),
        )(*passed, mix_bias)
        return jnp.transpose(result, (3, 0, 1, 2))

    return jax.shard_map(local_layers, mesh=mesh, in_specs=(vol_spec, P(), P(), P()), out_specs=vol_spec, check_vma=False)
```

```python
import functools

import jax
import jax.numpy as jnp
from jax import lax
from jax.experimental import pallas as pl
from jax.experimental.pallas import tpu as pltpu
from jax.sharding import PartitionSpec as P

PARTS_AXIS = "batch"
COL_AXIS = "ysp"
ROW_AXIS = "xsp"
H = 10
TAPS = 2 * H + 1
LAYERS = 3
C = 64
BX = 32
BY = 32
BZ = 32
ZL = 16
LANES = 128
CH = 8
NCH = BX // CH
QUAD = 4
NQ = BX // QUAD
WIN = CH + 2 * H
BEFORE = 5
EARLY = -(-(CH + H) // QUAD)
HEAD = QUAD + H
XS = BX + H
YS = BY + 2 * H
SEGS = ((BY - H, H), (0, H), (H, BY - 2 * H))
F32 = jnp.float32
BF16 = jnp.bfloat16


def band_times_eye(tap, rows, cols, inner, shift):
    i = lax.broadcasted_iota(jnp.int32, (rows, cols), 0)
    j = lax.broadcasted_iota(jnp.int32, (rows, cols), 1)
    t = j // inner - i // inner + shift
    acc = jnp.zeros((rows, cols), F32)
    for n in range(TAPS):
        acc = jnp.where(t == n, tap(n), acc)
    return jnp.where(i % inner == j % inner, acc, 0.0).astype(BF16)


def y_compute(window_of, old, put, ty, tz, w4, b, between=lambda stage: None):
    b = jnp.concatenate([b, b], axis=1)
    b = jnp.concatenate([b, b], axis=1)
    rs, ss = [], []
    for g in range(BY // 8):
        cols = [window_of(i, 8 * g).reshape(WIN * ZL, LANES) for i in range(QUAD)]
        rs.append(jnp.dot(ty[...], jnp.concatenate(cols, axis=1), preferred_element_type=F32).astype(BF16))
    between(0)
    for g in range(BY // 8):
        zs = []
        for i in range(QUAD):
            u = rs[g][:, LANES * i:LANES * (i + 1)].reshape(4, 2, ZL, LANES)
            ya, yb = u[:, 0], u[:, 1]
            lo = jnp.concatenate([ya[:, :, :C], yb[:, :, :C]], axis=2)
            hi = jnp.concatenate([ya[:, :, C:], yb[:, :, C:]], axis=2)
            zs.append(jnp.concatenate([lo, hi], axis=1).reshape(4 * BZ, LANES))
        dz = jnp.concatenate([jnp.concatenate(zs[:2], axis=0), jnp.concatenate(zs[2:], axis=0)], axis=1)
        ss.append(jnp.dot(tz[...], dz, preferred_element_type=F32).astype(BF16))
    between(1)
    for g in range(BY // 8):
        lhs = []
        for h in range(2):
            sh = ss[g][:, LANES * h:LANES * (h + 1)].reshape(8, 2, ZL, LANES)
            lhs.append(jnp.concatenate([sh[:, 0], sh[:, 1]], axis=2).reshape(8 * ZL, 2 * LANES))
        m = jnp.dot(jnp.concatenate(lhs, axis=0), w4[...], preferred_element_type=F32) + b
        m = jax.nn.gelu(m, approximate=True)
        for i in range(QUAD):
            mi = m[64 * i:64 * (i + 1)].reshape(4, 1, ZL, 2 * LANES)
            mi = jnp.concatenate([mi[..., :LANES], mi[..., LANES:]], axis=1).reshape(8, ZL, LANES)
            put(i, 8 * g, (old(i, 8 * g).astype(F32) + mi).astype(BF16))


def kernel(y_count, vol, taps_hbm, wmat_hbm, bias_hbm, out, u_out, ty_out, tz_out, w4_out, stage, vbuf, ubuf, tq, tx, ty, tz, w4, taps, wmat, bias, in_sem, small_sem, out_sem, ysend, yrecv, xsend, xrecv):
    xi = lax.axis_index(ROW_AXIS)
    yi = lax.axis_index(COL_AXIS)
    own = xi * H
    has_left = yi > 0
    has_right = yi < y_count - 1
    left = lax.rem(yi + y_count - 1, y_count)
    right = lax.rem(yi + 1, y_count)

    barrier = pltpu.get_barrier_semaphore()

    @pl.when(has_left)
    def _():
        pl.semaphore_signal(barrier, inc=1, device_id={COL_AXIS: left})

    @pl.when(has_right)
    def _():
        pl.semaphore_signal(barrier, inc=1, device_id={COL_AXIS: right})

    pl.semaphore_signal(barrier, inc=1, device_id={ROW_AXIS: 1 - xi})
    neighbours = 1 + has_left.astype(jnp.int32) + has_right.astype(jnp.int32)

    def x_of(k):
        return jnp.where(xi == 0, CH * k, BX - CH - CH * k)

    def xq_of(q):
        return jnp.where(xi == 0, QUAD * q, BX - QUAD - QUAD * q)

    x_head = jnp.where(xi == 0, 0, BX - HEAD)
    x_rest = jnp.where(xi == 0, HEAD, 0)

    def load(n):
        xs = pl.ds(x_rest, BX - HEAD) if n == 2 else pl.ds(x_head, HEAD)
        ys = pl.ds(0, BY) if n == 2 else pl.ds(*SEGS[min(n, 2)])
        return pltpu.make_async_copy(vol.at[xs, ys], stage.at[xs, ys], in_sem.at[n])

    small = [
        pltpu.make_async_copy(taps_hbm, taps, small_sem.at[0]),
        pltpu.make_async_copy(wmat_hbm, wmat, small_sem.at[1]),
        pltpu.make_async_copy(bias_hbm, bias, small_sem.at[2]),
    ]
    small[0].start()
    for n in range(4):
        load(n).start()
    small[1].start()
    small[2].start()

    def y_copy(l, q, side):
        xs = pl.ds(xq_of(q), QUAD)
        src = ubuf.at[l, xs, pl.ds(H, H)] if side == 0 else ubuf.at[l, xs, pl.ds(BY, H)]
        dst = ubuf.at[l, xs, pl.ds(H + BY, H)] if side == 0 else ubuf.at[l, xs, pl.ds(0, H)]
        return pltpu.make_async_remote_copy(
            src_ref=src, dst_ref=dst, send_sem=ysend.at[side], recv_sem=yrecv.at[l % 2, q],
            device_id={COL_AXIS: left if side == 0 else right})

    def x_copy(l):
        src = jnp.where(xi == 0, BX - H, H)
        dst = jnp.where(xi == 0, 0, BX)
        return pltpu.make_async_remote_copy(
            src_ref=vbuf.at[l, pl.ds(src, H)], dst_ref=vbuf.at[l, pl.ds(dst, H)],
            send_sem=xsend, recv_sem=xrecv.at[l % 2], device_id={ROW_AXIS: 1 - xi})

    def window(k):
        slot = own + x_of(k)
        return jnp.clip(slot - H, 0, XS - WIN), slot

    def x_mat(l, k):
        with jax.named_scope("xmat"):
            w0, slot = window(k)
            tx[...] = band_times_eye(lambda n: taps[l, 0, n], CH * ZL, WIN * ZL, ZL, w0 - slot + H)

    def x_rows(l, mat, w0, width, x0, count, seg):
        with jax.named_scope("xseg"):
            first, ny = SEGS[seg]
            cols = [vbuf[l, pl.ds(w0, width), first + i].reshape(width * ZL, LANES) for i in range(ny)]
            r = jnp.dot(mat, jnp.concatenate(cols, axis=1), preferred_element_type=F32).astype(BF16)
            for i in range(ny):
                ubuf[l, pl.ds(x0, count), H + first + i] = r[:, LANES * i:LANES * (i + 1)].reshape(count, ZL, LANES)

    def x_seg(l, k, seg):
        w0, _ = window(k)
        x_rows(l, tx[...], w0, WIN, x_of(k), CH, seg)

    def last_copy(side):
        l, q = LAYERS - 1, NQ - 1
        src = ubuf.at[l, pl.ds(xq_of(q), QUAD), pl.ds(H if side == 0 else BY, H)]
        return pltpu.make_async_remote_copy(
            src_ref=src, dst_ref=u_out.at[:, pl.ds(H + BY if side == 0 else 0, H)], send_sem=ysend.at[side], recv_sem=yrecv.at[l % 2, q],
            device_id={COL_AXIS: left if side == 0 else right})

    def send_quad(l, q, side):
        goes = has_left if side == 0 else has_right
        last = (l == LAYERS - 1) & (q == NQ - 1)

        @pl.when(goes & jnp.logical_not(last))
        def _():
            y_copy(l, q, side).start()

        @pl.when(goes & last)
        def _():
            last_copy(side).start()

    def y_send(l, k, side):
        for j in range(CH // QUAD):
            send_quad(l, k * (CH // QUAD) + j, side)

    def x_pass(l, k):
        x_mat(l, k)
        x_seg(l, k, 0)
        y_send(l, k, 1)
        x_seg(l, k, 1)
        y_send(l, k, 0)
        x_seg(l, k, 2)

    def layer_mats(l):
        ty[...] = band_times_eye(lambda n: taps[l, 1, n], CH * ZL, WIN * ZL, ZL, 0)
        i = lax.broadcasted_iota(jnp.int32, (8 * BZ, 8 * BZ), 0)
        j = lax.broadcasted_iota(jnp.int32, (8 * BZ, 8 * BZ), 1)
        t = j - i + H
        acc = jnp.zeros((8 * BZ, 8 * BZ), F32)
        for n in range(TAPS):
            acc = jnp.where(t == n, taps[l, 2, n], acc)
        tz[...] = jnp.where(i // BZ == j // BZ, acc, 0.0).astype(BF16)
        w = wmat[l].astype(F32)
        w = jnp.concatenate([w, w], axis=1)
        w = jnp.concatenate([w, w], axis=1)
        w = jnp.concatenate([w, w, w, w], axis=0)
        i = lax.broadcasted_iota(jnp.int32, (4 * C, 4 * C), 0) // C
        j = lax.broadcasted_iota(jnp.int32, (4 * C, 4 * C), 1) // C
        keep = (i // 2 == j % 2) & (i % 2 == j // 2)
        w4[...] = jnp.where(keep, w, 0.0).astype(BF16)

    def y_wait(l, q):
        with jax.named_scope("ywait"):
            both = ubuf.at[l, pl.ds(xq_of(q), QUAD), pl.ds(0, 2 * H)]

            @pl.when(has_left & has_right)
            def _():
                pltpu.make_async_remote_copy(
                    src_ref=both, dst_ref=both, send_sem=ysend.at[0], recv_sem=yrecv.at[l % 2, q],
                    device_id={COL_AXIS: left}).wait_recv()

            @pl.when(jnp.logical_not(has_left & has_right))
            def _():
                y_copy(l, q, 0).wait_recv()

    def y_quad(l, q):
        y_wait(l, q)
        with jax.named_scope("yquad"):
            xq = xq_of(q)
            nxt = jnp.minimum(l + 1, LAYERS - 1)

            def window_of(i, y0):
                return ubuf[l, xq + i, pl.ds(y0, WIN)]

            def old(i, y0):
                return vbuf[l, own + xq + i, pl.ds(y0, 8)]

            def put(i, y0, v):
                vbuf[nxt, own + xq + i, pl.ds(y0, 8)] = v

            y_compute(window_of, old, put, ty, tz, w4, bias[pl.ds(l, 1), :])

    def zero_planes(l):
        vbuf[l, pl.ds(own + jnp.where(xi == 0, QUAD * EARLY, 0), BX - QUAD * EARLY)] = jnp.zeros((BX - QUAD * EARLY, BY, ZL, LANES), BF16)

    def zero_halo(l, y0):
        def body(n, carry):
            ubuf[l, n, pl.ds(y0, H)] = jnp.zeros((H, ZL, LANES), BF16)
            return carry

        lax.fori_loop(0, BX, body, 0)

    def pack(n, x0, count, first, ny):
        with jax.named_scope("pack"):
            ys = pl.ds(first, ny)

            def body(p, c):
                s = stage[x0 + p, ys]
                vbuf[0, own + x0 + p, ys] = jnp.concatenate([s[:, :ZL], s[:, ZL:]], axis=2)
                return c

            lax.fori_loop(0, count, body, 0, unroll=True)

    small[0].wait()
    slot = own + xq_of(0)
    w0 = own + x_head
    tq[...] = band_times_eye(lambda n: taps[0, 0, n], QUAD * ZL, HEAD * ZL, ZL, w0 - slot + H)
    for seg in range(2):
        load(seg).wait()
        pack(seg, x_head, HEAD, *SEGS[seg])
        x_rows(0, tq[...], w0, HEAD, xq_of(0), QUAD, seg)
        if seg == 0:
            with jax.named_scope("barrier"):
                pl.semaphore_wait(barrier, neighbours)
        send_quad(0, 0, 1 - seg)
    x_mat(0, 0)
    load(2).wait()
    pack(2, x_rest, BX - HEAD, 0, BY)
    x_copy(0).start()
    second = tx[pl.ds(jnp.where(xi == 0, QUAD * ZL, 0), QUAD * ZL), :]
    for seg in range(2):
        x_rows(0, second, window(0)[0], WIN, xq_of(1), QUAD, seg)
        send_quad(0, 1, 1 - seg)
    load(3).wait()
    pack(3, x_head, HEAD, *SEGS[2])
    x_seg(0, 0, 2)
    x_pass(0, 1)
    for l in range(1, LAYERS):
        zero_planes(l)
    small[1].wait()
    small[2].wait()

    def layer(l, carry):
        def xs(k, c):
            @pl.when(k == 2)
            def _():
                with jax.named_scope("xwait"):
                    x_copy(l).wait()

            x_pass(l, k)
            return c

        lax.fori_loop(2, NCH, xs, 0)
        with jax.named_scope("mats"):
            layer_mats(l)

        @pl.when(jnp.logical_not(has_left))
        def _():
            zero_halo(l, 0)

        @pl.when(jnp.logical_not(has_right))
        def _():
            zero_halo(l, H + BY)

        @pl.when(l == LAYERS - 1)
        def _():
            store(NQ - 1).start()
            for mat in store_mats:
                mat.start()
            store_u.start()
            for edge, copy in store_edges:
                pl.when(edge)(copy.start)

        def ys(q, c):
            @pl.when(((q == EARLY) | (q == NQ - 1)) & (l < LAYERS - 1))
            def _():
                x_pass(l + 1, jnp.where(q == EARLY, 0, 1))

            @pl.when((q < NQ - 1) | (l < LAYERS - 1))
            def _():
                y_quad(l, q)

            @pl.when((q < NQ - 1) & (l == LAYERS - 1))
            def _():
                store(q).start()

            return c

        lax.fori_loop(0, NQ, ys, 0)

        @pl.when(l < LAYERS - 1)
        def _():
            x_copy(l + 1).start()

        return carry

    def store(q):
        xs = xq_of(q)
        return pltpu.make_async_copy(vbuf.at[LAYERS - 1, pl.ds(own + xs, QUAD)], out.at[pl.ds(xs, QUAD)], out_sem)

    store_mats = [pltpu.make_async_copy(m, o, small_sem.at[n]) for n, (m, o) in enumerate(((ty, ty_out), (tz, tz_out), (w4, w4_out)))]
    last_u = ubuf.at[LAYERS - 1, pl.ds(xq_of(NQ - 1), QUAD)]
    store_u = pltpu.make_async_copy(last_u.at[:, pl.ds(H, BY)], u_out.at[:, pl.ds(H, BY)], in_sem.at[0])
    store_edges = [
        (jnp.logical_not(has), pltpu.make_async_copy(last_u.at[:, pl.ds(y0, H)], u_out.at[:, pl.ds(y0, H)], in_sem.at[n]))
        for has, y0, n in ((has_left, 0, 2), (has_right, H + BY, 3))
    ]
    lax.fori_loop(0, LAYERS, layer, 0)
    y_wait(LAYERS - 1, NQ - 1)

    with jax.named_scope("finish"):
        for side in range(2):
            sent = ubuf.at[:, :, pl.ds(0, H)]

            @pl.when(has_left if side == 0 else has_right)
            def _():
                pltpu.make_async_remote_copy(
                    src_ref=sent, dst_ref=sent, send_sem=ysend.at[side], recv_sem=yrecv.at[0, 0],
                    device_id={COL_AXIS: left if side == 0 else right}).wait_send()

        pltpu.make_async_copy(vbuf.at[LAYERS - 1, pl.ds(own, BX)], out, out_sem).wait()
        for edge, copy in store_edges:
            pl.when(edge)(copy.wait)
        for mat in store_mats:
            mat.wait()
        store_u.wait()


def unpack(s):
    r = pltpu.roll(s.reshape(QUAD * BY * ZL, LANES), C, 1).reshape(QUAD, BY, ZL, LANES)
    return s[:, :, :, :C], r[:, :, :, :C]


def last_kernel(src, u_hbm, ty_hbm, tz_hbm, w4_hbm, bias_hbm, dst, got, u, ty, tz, w4, bias, buf, in_sems, mat_sems, out_sem):
    xi = lax.axis_index(ROW_AXIS)

    def planes(q):
        return pl.ds(jnp.where(xi == 0, QUAD * q, BX - QUAD - QUAD * q), QUAD)

    def read(q):
        return pltpu.make_async_copy(src.at[planes(q)], got.at[planes(q)], in_sems.at[q])

    def write(q):
        return pltpu.make_async_copy(buf.at[planes(q)], dst.at[planes(q)], out_sem)

    mats = [
        pltpu.make_async_copy(h, v, mat_sems.at[n])
        for n, (h, v) in enumerate(((u_hbm, u), (ty_hbm, ty), (tz_hbm, tz), (w4_hbm, w4), (bias_hbm, bias)))
    ]
    for q in range(NQ - 1):
        read(q).start()
    for mat in mats:
        mat.start()
    read(NQ - 1).start()

    def turn(q):
        buf[planes(q), :, :ZL, :], buf[planes(q), :, ZL:, :] = unpack(got[planes(q)])

    def body(q, carry):
        read(q).wait()
        turn(q)
        write(q).start()
        return carry

    def between(stage):
        for q in range(BEFORE, NQ - 1):
            if stage == 0:
                turn(q)
            else:
                write(q).start()

    with jax.named_scope("unpack"):
        lax.fori_loop(0, BEFORE, body, 0)
        for q in range(BEFORE, NQ - 1):
            read(q).wait()
    with jax.named_scope("matwait"):
        for mat in mats:
            mat.wait()
        read(NQ - 1).wait()
    xq = jnp.where(xi == 0, BX - QUAD, 0)

    def put(i, y0, v):
        buf[xq + i, pl.ds(y0, 8), :ZL, :] = v[:, :, :C]
        buf[xq + i, pl.ds(y0, 8), ZL:, :] = v[:, :, C:]

    with jax.named_scope("ycomp"):
        y_compute(
            lambda i, y0: u[i, pl.ds(y0, WIN)], lambda i, y0: got[xq + i, pl.ds(y0, 8)], put,
            ty, tz, w4, bias[pl.ds(LAYERS - 1, 1), :], between)
    write(NQ - 1).start()

    with jax.named_scope("outwait"):
        pltpu.make_async_copy(buf, dst, out_sem).wait()


def solution(mesh):
    y_count = mesh.shape[COL_AXIS]
    vol_spec = P(PARTS_AXIS, ROW_AXIS, COL_AXIS, None)
    any_spec = pl.BlockSpec(memory_space=pl.ANY)

    def local_layers(volume, filter_taps, mix_weights, mix_bias):
        vol = jnp.transpose(volume, (1, 2, 3, 0))
        toeplitz = (CH * ZL, WIN * ZL)
        passed_shapes = ((BX, BY, ZL, LANES), (QUAD, YS, ZL, LANES), toeplitz, (8 * BZ, 8 * BZ), (4 * C, 4 * C))
        passed = pl.pallas_call(
            functools.partial(kernel, y_count),
            out_shape=[jax.ShapeDtypeStruct(shape, BF16) for shape in passed_shapes],
            in_specs=[any_spec] * 4,
            out_specs=[any_spec] * 5,
            scratch_shapes=[
                pltpu.VMEM((BX, BY, BZ, C), BF16),
                pltpu.VMEM((LAYERS, XS, BY, ZL, LANES), BF16),
                pltpu.VMEM((LAYERS, BX, YS, ZL, LANES), BF16),
                pltpu.VMEM((QUAD * ZL, HEAD * ZL), BF16),
                pltpu.VMEM(toeplitz, BF16),
                pltpu.VMEM(toeplitz, BF16),
                pltpu.VMEM((8 * BZ, 8 * BZ), BF16),
                pltpu.VMEM((4 * C, 4 * C), BF16),
                pltpu.SMEM((LAYERS, 3, TAPS), F32),
                pltpu.VMEM((LAYERS, C, C), BF16),
                pltpu.VMEM((LAYERS, C), F32),
                pltpu.SemaphoreType.DMA((4,)),
                pltpu.SemaphoreType.DMA((3,)),
                pltpu.SemaphoreType.DMA,
                pltpu.SemaphoreType.DMA((2,)),
                pltpu.SemaphoreType.DMA((2, NQ)),
                pltpu.SemaphoreType.DMA,
                pltpu.SemaphoreType.DMA((2,)),
            ],
            compiler_params=pltpu.CompilerParams(collective_id=0, has_side_effects=True, vmem_limit_bytes=60 * 2**20),
        )(vol, filter_taps, mix_weights, mix_bias)
        result = pl.pallas_call(
            last_kernel,
            out_shape=jax.ShapeDtypeStruct((BX, BY, BZ, C), BF16),
            in_specs=[any_spec] * 6,
            out_specs=any_spec,
            scratch_shapes=[pltpu.VMEM(shape, BF16) for shape in passed_shapes] + [
                pltpu.VMEM((LAYERS, C), F32),
                pltpu.VMEM((BX, BY, BZ, C), BF16),
                pltpu.SemaphoreType.DMA((NQ,)),
                pltpu.SemaphoreType.DMA((5,)),
                pltpu.SemaphoreType.DMA,
            ],
            compiler_params=pltpu.CompilerParams(vmem_limit_bytes=60 * 2**20),
        )(*passed, mix_bias)
        return jnp.transpose(result, (3, 0, 1, 2))

    return jax.shard_map(local_layers, mesh=mesh, in_specs=(vol_spec, P(), P(), P()), out_specs=vol_spec, check_vma=False)
```
